32 devices in a mesh: shot: 8 (over z, y), depth: 4 (over x, core).
Axes of the slice: x: 2, y: 2, z: 4, core: 2. Of those that a mesh axis runs over, the one named last changes fastest.
Arguments:
- correlation: float32 [16, 16, 32, 512], P('shot', None, None, 'depth'), may hold values from -6 to 6
- illumination: float32 [16, 16, 32, 512], P('shot', None, None, 'depth'), may hold values from 0.25 to 4
- aperture: int32 [16, 4], P('shot'), may hold values from 0 to 32, as said below
Outputs:
- stack: float32 [16, 32, 512], P('shot', None, 'depth')
The draws below stay inside these ranges and needn't reach their ends.
Inputs may be any that keep to these rules, and one draw needn't show every extreme that they name: For every shot, 0 <= aperture[s,0] < aperture[s,1] <= 16 and 0 <= aperture[s,2] < aperture[s,3] <= 32; each box spans a quarter to a half of the grid along each of the two dimensions.
All inputs are finite; a program needn't handle non-finite values.
Results may differ from the reference program's by a relative error of at most 0.0003.
Values sent between devices are 32-bit elements.
No kernel may reach another device: no remote copies, remote signals or barrier semaphores. Data moves between devices by JAX's collectives and lax.ppermute only.
A program may use at most 64 MiB of HBM per device.

```python
import math
import jax
import jax.numpy as jnp
from jax import lax

NY = 32
SHOTS = 16
NX = 16
NZ = 512


def draw_aperture(key, part):
    key_first = jax.random.fold_in(key, 11)
    key_second = jax.random.fold_in(key, 23)
    k_one, k_two = jax.random.split(key_first)
    k_three, k_four = jax.random.split(key_second)
    low_first = jax.random.randint(k_one, (SHOTS,), 0, NX // 2)
    span_first = jax.random.randint(k_two, (SHOTS,), max(NX // 4, 1), NX // 2 + 1)
    low_second = jax.random.randint(k_three, (SHOTS,), 0, NY // 2)
    span_second = jax.random.randint(k_four, (SHOTS,), max(NY // 4, 1), NY // 2 + 1)
    return jnp.stack([low_first, low_first + span_first, low_second, low_second + span_second], axis=1).astype(jnp.int32)


def spiked(values, rng, source, target, blocks, factor):
    owner, partner = [(jnp.arange(values.shape[position]) // (values.shape[position] // blocks)).reshape([-1 if axis == position else 1 for axis in range(values.ndim)]) for position in (source, target)]
    chosen = jax.random.permutation(rng, blocks)[partner]
    strong = (owner == chosen) | (owner == (partner + blocks // 2) % blocks)
    return jnp.where(strong, factor * values, values)


def steps_of(stream_key, dims, pieces, smallest, high):
    def one(dim, blocks):
        draws = jax.random.uniform(jax.random.fold_in(jax.random.fold_in(stream_key, 6), dim), (blocks,), jnp.float32, smallest / len(pieces), high / len(pieces))
        return jnp.repeat(jnp.exp(draws), dims[dim] // blocks).reshape((-1,) + (1,) * (len(dims) - dim - 1))

    gain = one(*pieces[0])
    for cut in pieces[1:]:
        gain = gain * one(*cut)
    return gain


def gaussian_with(stream_key, dims, width, most, pieces, heavy, kind=jnp.bfloat16):
    array = width * jax.random.normal(stream_key, dims, jnp.float32)
    if pieces:
        array = array * steps_of(stream_key, dims, pieces, -0.22, 0.18)
    return jnp.clip(spiked(array, jax.random.fold_in(stream_key, 3), *heavy), -most, most).astype(kind)


def setup_inputs(seed: int = 0) -> dict:
    seeds = jax.random.split(jax.random.key(seed), 4)
    correlation = gaussian_with(seeds[0], (SHOTS, NX, NY, NZ), 1.0, 6.0, ((0, 8), (3, 4)), (0, 1, 8, 2.0), jnp.float32)
    illumination = jnp.clip(jnp.exp(math.log(4.0) - 2.7725887 * jax.random.uniform(seeds[1], (SHOTS, NX, NY, NZ), jnp.float32) ** steps_of(seeds[1], (SHOTS, NX, NY, NZ), ((0, 8), (3, 4)), -0.2, 0.2)), 0.25, 4.0)
    aperture = draw_aperture(jax.random.fold_in(seeds[3], 71), 0)
    return {"correlation": correlation, "illumination": illumination, "aperture": aperture}


def negative_laplacian(field):
    padded = jnp.pad(field, 1)
    beside = padded[2:, 1:-1, 1:-1] + padded[:-2, 1:-1, 1:-1]
    beside = beside + padded[1:-1, 2:, 1:-1] + padded[1:-1, :-2, 1:-1]
    beside = beside + padded[1:-1, 1:-1, 2:] + padded[1:-1, 1:-1, :-2]
    return 6.0 * field - beside

def prepare(correlation, illumination, box):
    first = lax.broadcasted_iota(jnp.int32, (NX, NY, 1), 0)
    second = lax.broadcasted_iota(jnp.int32, (NX, NY, 1), 1)
    inside = (first >= box[0]) & (first < box[1]) & (second >= box[2]) & (second < box[3])
    mask = inside.astype(jnp.float32)
    return negative_laplacian(mask * correlation / (illumination + 0.1))

def reference(correlation, illumination, aperture):
    cells = NX * NY * NZ

    def energy(items):
        filtered = prepare(items[0], items[1], items[2])
        return jnp.sum(filtered * filtered) / cells
    meansq = lax.map(energy, (correlation, illumination, aperture))
    peak = jnp.max(meansq)
    weight = 1.0 / jnp.sqrt(meansq + 0.5 * peak + 1.0)

    def accumulate(total, items):
        filtered = prepare(items[0], items[1], items[2])
        return (total + items[3] * filtered, None)
    stack, unused = lax.scan(accumulate, jnp.zeros((NX, NY, NZ), jnp.float32), (correlation, illumination, aperture, weight))
    return stack / jnp.sqrt(jnp.float32(SHOTS))
```

```python
import math

import jax
import jax.numpy as jnp
from jax import lax
from jax.experimental import pallas as pl
from jax.experimental.pallas import tpu as pltpu
from jax.sharding import PartitionSpec as P


def local_filter_kernel(aperture, correlation, illumination, partial, first_edge, last_edge, padded):
    shots, rows, cols, slab = correlation.shape
    second = lax.broadcasted_iota(jnp.int32, (cols, slab), 0)
    lane = lax.broadcasted_iota(jnp.int32, (cols, slab), 1)
    zero = jnp.zeros((cols, slab), jnp.float32)
    group = 128 // cols
    for s in range(shots):
        padded[0] = zero
        padded[rows + 1] = zero
        in_cols = (second >= aperture[s, 2]) & (second < aperture[s, 3])
        for x in range(rows):
            keep = in_cols & (x >= aperture[s, 0]) & (x < aperture[s, 1])
            padded[x + 1] = jnp.where(keep, correlation[s, x] / (illumination[s, x] + 0.1), 0.0)
        for c in range(rows // group):
            turned = padded[c * group + 1 : (c + 1) * group + 1].reshape(group * cols, slab).T
            at = s * (rows // group) + c
            first_edge[at : at + 1] = turned[0:1]
            last_edge[at : at + 1] = turned[slab - 1 : slab]
        for x in range(rows):
            n = padded[x + 1]
            beside = padded[x] + padded[x + 2]
            beside += jnp.where(second == 0, 0.0, pltpu.roll(n, 1, 0))
            beside += jnp.where(second == cols - 1, 0.0, pltpu.roll(n, cols - 1, 0))
            beside += jnp.where(lane == 0, 0.0, pltpu.roll(n, 1, 1))
            beside += jnp.where(lane == slab - 1, 0.0, pltpu.roll(n, slab - 1, 1))
            partial[s, x] = 6.0 * n - beside


def finish_filter_kernel(partial, low, high, filtered, energy):
    shots, rows, cols, slab = partial.shape
    owners, _, own = filtered.shape[:3]
    group = 128 // cols
    depth = lax.broadcasted_iota(jnp.int32, (slab, 128), 0)
    for s in range(shots):
        total = jnp.zeros((cols, slab), jnp.float32)
        for c in range(rows // group):
            at = s * (rows // group) + c
            halo = jnp.where(depth == 0, low[at : at + 1], jnp.where(depth == slab - 1, high[at : at + 1], 0.0)).T
            for g in range(group):
                x = c * group + g
                value = partial[s, x] - halo[g * cols : (g + 1) * cols]
                filtered[x // own, s, x % own] = value
                total += value * value
        energy[:, s : s + 1, :] = jnp.broadcast_to(jnp.sum(total, axis=0, keepdims=True)[None], (energy.shape[0], 1, slab))


def combine_kernel(cells, total_shots, energy, filtered, stack):
    owners, shots, own, cols, slab = filtered.shape
    slabs = energy.shape[0] // owners
    sums = []
    for g in range(owners):
        part = energy[g * slabs]
        for d in range(1, slabs):
            part = part + energy[g * slabs + d]
        sums.append(part)
    meansq = jnp.sum(jnp.concatenate(sums, axis=0), axis=1, keepdims=True) / cells
    peak = jnp.max(meansq, axis=0, keepdims=True)
    weight = (1.0 / math.sqrt(total_shots)) / jnp.sqrt(meansq + 0.5 * peak + 1.0)
    weight = jnp.broadcast_to(weight, (owners * shots, slab))
    for j in range(own):
        acc = jnp.zeros((cols, slab), jnp.float32)
        for g in range(owners):
            for s in range(shots):
                at = g * shots + s
                acc += weight[at : at + 1] * filtered[g, s, j]
        stack[j] = acc


def on_device(correlation, illumination, aperture):
    shots, rows, cols, slab = correlation.shape
    owners, slabs = lax.axis_size("shot"), lax.axis_size("depth")
    own = rows // owners
    f32 = jnp.float32
    vmem = pl.BlockSpec(memory_space=pltpu.VMEM)
    smem = pl.BlockSpec(memory_space=pltpu.SMEM)
    edge = jax.ShapeDtypeStruct((shots * rows * cols // 128, 128), f32)
    partial, first_edge, last_edge = pl.pallas_call(
        local_filter_kernel,
        out_shape=(jax.ShapeDtypeStruct(correlation.shape, f32), edge, edge),
        in_specs=[smem, vmem, vmem],
        out_specs=(vmem, vmem, vmem),
        scratch_shapes=[pltpu.VMEM((rows + 2, cols, slab), f32)],
        name="local_filter",
    )(aperture, correlation, illumination)
    forward = [(i, i + 1) for i in range(slabs - 1)]
    low = lax.ppermute(last_edge, "depth", forward)
    high = lax.ppermute(first_edge, "depth", [(b, a) for a, b in forward])
    filtered, energy = pl.pallas_call(
        finish_filter_kernel,
        out_shape=(
            jax.ShapeDtypeStruct((owners, shots, own, cols, slab), f32),
            jax.ShapeDtypeStruct((owners * slabs, shots, slab), f32),
        ),
        in_specs=[vmem, vmem, vmem],
        out_specs=(vmem, vmem),
        name="finish_filter",
    )(partial, low, high)
    filtered = lax.all_to_all(filtered, "shot", 0, 0, tiled=True)
    energy = lax.all_to_all(energy, ("shot", "depth"), 0, 0, tiled=True)
    cells = rows * cols * slab * slabs

    def body(*refs):
        combine_kernel(cells, shots * owners, *refs)

    return pl.pallas_call(
        body,
        out_shape=jax.ShapeDtypeStruct((own, cols, slab), f32),
        in_specs=[vmem, vmem],
        out_specs=vmem,
        name="combine",
    )(energy, filtered)


def solution(mesh):
    return jax.shard_map(
        on_device,
        mesh=mesh,
        in_specs=(P("shot", None, None, "depth"), P("shot", None, None, "depth"), P("shot", None)),
        out_specs=P("shot", None, "depth"),
        check_vma=False,
    )
```

```python
import math

import jax
import jax.numpy as jnp
from jax import lax
from jax.experimental import pallas as pl
from jax.experimental.pallas import tpu as pltpu
from jax.sharding import PartitionSpec as P


def local_filter_kernel(
    aperture, correlation_hbm, illumination_hbm, partial, first_edge, last_edge, padded, correlation, illumination, arrived
):
    shots, rows, cols, slab = correlation.shape
    owners = first_edge.shape[0]
    own = rows // owners
    copies = []
    for s in range(shots):
        copies.append((
            pltpu.make_async_copy(correlation_hbm.at[s], correlation.at[s], arrived.at[0, s]),
            pltpu.make_async_copy(illumination_hbm.at[s], illumination.at[s], arrived.at[1, s]),
        ))
        for copy in copies[s]:
            copy.start()
    second = lax.broadcasted_iota(jnp.int32, (cols, slab), 0)
    lane = lax.broadcasted_iota(jnp.int32, (cols, slab), 1)
    zero = jnp.zeros((cols, slab), jnp.float32)
    for s in range(shots):
        padded[s, 0] = zero
        padded[s, rows + 1] = zero
        for copy in copies[s]:
            copy.wait()
        in_cols = (second >= aperture[s, 2]) & (second < aperture[s, 3])
        for x in range(rows):
            keep = in_cols & (x >= aperture[s, 0]) & (x < aperture[s, 1])
            padded[s, x + 1] = jnp.where(keep, correlation[s, x] / (illumination[s, x] + 0.1), 0.0)
        for x in range(rows):
            n = padded[s, x + 1]
            beside = padded[s, x] + padded[s, x + 2]
            beside += jnp.where(second == 0, 0.0, pltpu.roll(n, 1, 0))
            beside += jnp.where(second == cols - 1, 0.0, pltpu.roll(n, cols - 1, 0))
            beside += jnp.where(lane == 0, 0.0, pltpu.roll(n, 1, 1))
            beside += jnp.where(lane == slab - 1, 0.0, pltpu.roll(n, slab - 1, 1))
            partial[s, x] = 6.0 * n - beside
    for r in range(owners):
        held = jnp.concatenate([padded[s, x + 1] for s in range(shots) for x in range(r * own, (r + 1) * own)], axis=0)
        turned = held.T
        first_edge[r : r + 1] = turned[0:1]
        last_edge[r : r + 1] = turned[slab - 1 : slab]


def finish_filter_kernel(mine, partial, low, high, energy, *blocks):
    shots, rows, cols, slab = partial.shape
    owners = len(blocks)
    own = rows // owners
    depth = lax.broadcasted_iota(jnp.int32, (slab, shots * own * cols), 0)
    totals = [jnp.zeros((cols, slab), jnp.float32) for _ in range(shots)]
    for k in range(owners):
        r = mine[0] ^ k
        halo = jnp.where(depth == 0, low[pl.ds(r, 1)], jnp.where(depth == slab - 1, high[pl.ds(r, 1)], 0.0)).T
        for s in range(shots):
            for j in range(own):
                at = (s * own + j) * cols
                value = partial[s, r * own + j] - halo[at : at + cols]
                blocks[k][s, j] = value
                totals[s] += value * value
    for s in range(shots):
        summed = jnp.sum(totals[s], axis=0, keepdims=True)
        energy[:, s : s + 1, :] = jnp.broadcast_to(summed[None], (energy.shape[0], 1, slab))


def combine_kernel(cells, total_shots, mine, energy, stack, weights, *blocks):
    owners = len(blocks)
    shots, own, cols, slab = blocks[0].shape
    slabs = energy.shape[0] // owners
    sums = []
    for g in range(owners):
        part = energy[g * slabs]
        for d in range(1, slabs):
            part = part + energy[g * slabs + d]
        sums.append(part)
    meansq = jnp.sum(jnp.concatenate(sums, axis=0), axis=1, keepdims=True) / cells
    peak = jnp.max(meansq, axis=0, keepdims=True)
    weight = (1.0 / math.sqrt(total_shots)) / jnp.sqrt(meansq + 0.5 * peak + 1.0)
    weights[...] = jnp.broadcast_to(weight, (owners * shots, slab))
    for j in range(own):
        acc = jnp.zeros((cols, slab), jnp.float32)
        for k in range(owners):
            for s in range(shots):
                acc += weights[pl.ds((mine[0] ^ k) * shots + s, 1)] * blocks[k][s, j]
        stack[j] = acc


def in_hbm(array):
    return pltpu.with_memory_space_constraint(array, pltpu.HBM)


def in_vmem(array):
    return pltpu.with_memory_space_constraint(array, pltpu.VMEM)


def on_device(correlation, illumination, aperture):
    shots, rows, cols, slab = correlation.shape
    owners, slabs = lax.axis_size("shot"), lax.axis_size("depth")
    assert owners & (owners - 1) == 0 and rows % owners == 0
    own = rows // owners
    f32 = jnp.float32
    vmem = pl.BlockSpec(memory_space=pltpu.VMEM)
    hbm = pl.BlockSpec(memory_space=pltpu.HBM)
    smem = pl.BlockSpec(memory_space=pltpu.SMEM)
    params = pltpu.CompilerParams(vmem_limit_bytes=16 << 20)
    edge = pltpu.VMEM((owners, shots * own * cols), f32)
    mine = lax.axis_index("shot").reshape(1)
    partial, first_edge, last_edge = pl.pallas_call(
        local_filter_kernel,
        out_shape=(pltpu.VMEM(correlation.shape, f32), edge, edge),
        in_specs=[smem, hbm, hbm],
        out_specs=(vmem, vmem, vmem),
        scratch_shapes=[
            pltpu.VMEM((shots, rows + 2, cols, slab), f32),
            pltpu.VMEM(correlation.shape, f32),
            pltpu.VMEM(correlation.shape, f32),
            pltpu.SemaphoreType.DMA((2, shots)),
        ],
        compiler_params=params,
        name="local_filter",
    )(aperture, in_hbm(correlation), in_hbm(illumination))
    forward = [(i, i + 1) for i in range(slabs - 1)]
    low = lax.ppermute(last_edge, "depth", forward)
    high = lax.ppermute(first_edge, "depth", [(b, a) for a, b in forward])
    energy, *blocks = pl.pallas_call(
        finish_filter_kernel,
        out_shape=(pltpu.VMEM((owners * slabs, shots, slab), f32),)
        + (pltpu.VMEM((shots, own, cols, slab), f32),) * owners,
        in_specs=[smem, vmem, vmem, vmem],
        out_specs=(vmem,) * (1 + owners),
        compiler_params=params,
        name="finish_filter",
    )(mine, *(in_vmem(v) for v in (partial, low, high)))
    energy = lax.all_to_all(energy, ("shot", "depth"), 0, 0, tiled=True)
    for k in range(1, owners):
        blocks[k] = lax.ppermute(blocks[k], "shot", [(i, i ^ k) for i in range(owners)])
    cells = rows * cols * slab * slabs

    def body(mine, energy, *refs):
        combine_kernel(cells, shots * owners, mine, energy, refs[owners], refs[owners + 1], *refs[:owners])

    return pl.pallas_call(
        body,
        out_shape=jax.ShapeDtypeStruct((own, cols, slab), f32),
        in_specs=[smem] + [vmem] * (1 + owners),
        out_specs=vmem,
        scratch_shapes=[pltpu.VMEM((owners * shots, slab), f32)],
        compiler_params=params,
        name="combine",
    )(mine, *(in_vmem(v) for v in (energy, *blocks)))


def solution(mesh):
    return jax.shard_map(
        on_device,
        mesh=mesh,
        in_specs=(P("shot", None, None, "depth"), P("shot", None, None, "depth"), P("shot", None)),
        out_specs=P("shot", None, "depth"),
        check_vma=False,
    )
```

```python
import math

import jax
import jax.numpy as jnp
from jax import lax
from jax.experimental import pallas as pl
from jax.experimental.pallas import tpu as pltpu
from jax.sharding import PartitionSpec as P


def local_filter_kernel(
    aperture_hbm, correlation_hbm, illumination_hbm, partial, message, padded, correlation, illumination, aperture, arrived, read
):
    shots, rows, cols, slab = correlation.shape
    own = message.shape[1] // (shots * cols)
    owners = rows // own
    boxes = pltpu.make_async_copy(aperture_hbm, aperture, read)
    boxes.start()
    copies = []
    for s in range(shots):
        copies.append((
            pltpu.make_async_copy(correlation_hbm.at[s], correlation.at[s], arrived.at[0, s]),
            pltpu.make_async_copy(illumination_hbm.at[s], illumination.at[s], arrived.at[1, s]),
        ))
        for copy in copies[s]:
            copy.start()
    second = lax.broadcasted_iota(jnp.int32, (cols, slab), 0)
    lane = lax.broadcasted_iota(jnp.int32, (cols, slab), 1)
    zero = jnp.zeros((cols, slab), jnp.float32)
    boxes.wait()
    for s in range(shots):
        padded[s, 0] = zero
        padded[s, rows + 1] = zero
        for copy in copies[s]:
            copy.wait()
        in_cols = (second >= aperture[s, 2]) & (second < aperture[s, 3])
        for x in range(rows):
            keep = in_cols & (x >= aperture[s, 0]) & (x < aperture[s, 1])
            padded[s, x + 1] = jnp.where(keep, correlation[s, x] / (illumination[s, x] + 0.1), 0.0)
        total = zero
        for x in range(rows):
            n = padded[s, x + 1]
            beside = padded[s, x] + padded[s, x + 2]
            beside += jnp.where(second == 0, 0.0, pltpu.roll(n, 1, 0))
            beside += jnp.where(second == cols - 1, 0.0, pltpu.roll(n, cols - 1, 0))
            beside += jnp.where(lane == 0, 0.0, pltpu.roll(n, 1, 1))
            beside += jnp.where(lane == slab - 1, 0.0, pltpu.roll(n, slab - 1, 1))
            value = 6.0 * n - beside
            partial[s, x] = value
            total += value * value
        message[4 * owners + s : 4 * owners + s + 1] = jnp.sum(total, axis=0, keepdims=True)
    for r in range(owners):
        for at, image, shift in ((0, padded, 1), (2 * owners, partial, 0)):
            held = [image[s, r * own + j + shift] for s in range(shots) for j in range(own)]
            turned = jnp.concatenate(held, axis=0).T
            message[at + r : at + r + 1] = turned[0:1]
            message[at + owners + r : at + owners + r + 1] = turned[slab - 1 : slab]


def finish_filter_kernel(aperture, place, partial, messages, blocks, slabs_held, filtered):
    shots, rows, cols, slab = partial.shape
    owners, slabs = len(blocks), len(messages)
    own = rows // owners
    window = cols // 2 + 2
    width = shots * own * cols
    here = place[1]
    for k in range(slabs):
        slabs_held[here ^ k] = messages[k][...]
    cross = jnp.zeros((owners, width), jnp.float32)
    for d in range(slabs - 1):
        right = slabs_held[d + 1, 0:owners]
        left = slabs_held[d, owners : 2 * owners]
        cross += right * (right - 2.0 * slabs_held[d, 3 * owners : 4 * owners])
        cross += left * (left - 2.0 * slabs_held[d + 1, 2 * owners : 3 * owners])
    cross = jnp.sum(cross, axis=0, keepdims=True)
    lane = lax.broadcasted_iota(jnp.int32, (1, width), 1)
    tails = []
    starts = []
    for s in range(shots):
        energy = jnp.where((lane >= s * own * cols) & (lane < (s + 1) * own * cols), cross, 0.0)
        for d in range(slabs):
            energy += slabs_held[d, 4 * owners + s : 4 * owners + s + 1]
        tails.append(energy)
    for s in range(shots):
        starts.append(jnp.clip(aperture[s, 2] - 1, 0, cols - window))
        tails.append(jnp.full((1, width), starts[s].astype(jnp.float32)))
    tail = jnp.concatenate(tails, axis=0)
    depth = lax.broadcasted_iota(jnp.int32, (slab, width), 0)
    below = jnp.maximum(here - 1, 0)
    above = jnp.minimum(here + 1, slabs - 1)
    has_below = (depth == 0) & (here > 0)
    has_above = (depth == slab - 1) & (here < slabs - 1)
    for k in range(owners):
        r = place[0] ^ k
        low = slabs_held[below, pl.ds(owners + r, 1)]
        high = slabs_held[above, pl.ds(r, 1)]
        halo = jnp.where(has_below, low, jnp.where(has_above, high, 0.0)).T
        for s in range(shots):
            for j in range(own):
                i = s * own + j
                filtered[k, i] = partial[s, r * own + j] - halo[i * cols : (i + 1) * cols]
                blocks[k][i * window : (i + 1) * window] = filtered[k, i, pl.ds(starts[s], window)]
        blocks[k][shots * own * window :] = tail


def combine_kernel(cells, total_shots, shots, blocks, stack, weights):
    owners = len(blocks)
    own, cols, slab = stack.shape
    window = cols // 2 + 2
    tail = shots * own * window
    energy = jnp.concatenate([block[tail : tail + shots] for block in blocks], axis=0)
    meansq = jnp.sum(energy, axis=1, keepdims=True) / cells
    peak = jnp.max(meansq, axis=0, keepdims=True)
    weight = (1.0 / math.sqrt(total_shots)) / jnp.sqrt(meansq + 0.5 * peak + 1.0)
    weights[...] = jnp.broadcast_to(weight, (owners * shots, slab))
    stack[...] = jnp.zeros(stack.shape, jnp.float32)
    for k in range(owners):
        for s in range(shots):
            start = jnp.max(blocks[k][tail + shots + s : tail + shots + s + 1]).astype(jnp.int32)
            scale = weights[k * shots + s : k * shots + s + 1]
            for j in range(own):
                i = s * own + j
                stack[j, pl.ds(start, window)] += scale * blocks[k][i * window : (i + 1) * window]


def in_hbm(array):
    return pltpu.with_memory_space_constraint(array, pltpu.HBM)


def in_vmem(array):
    return pltpu.with_memory_space_constraint(array, pltpu.VMEM)


def on_device(correlation, illumination, aperture):
    shots, rows, cols, slab = correlation.shape
    owners, slabs = lax.axis_size("shot"), lax.axis_size("depth")
    assert owners & (owners - 1) == 0 and slabs & (slabs - 1) == 0 and rows % owners == 0
    own = rows // owners
    width = shots * own * cols
    assert width == slab == 128
    f32 = jnp.float32
    vmem = pl.BlockSpec(memory_space=pltpu.VMEM)
    hbm = pl.BlockSpec(memory_space=pltpu.HBM)
    smem = pl.BlockSpec(memory_space=pltpu.SMEM)
    params = pltpu.CompilerParams(vmem_limit_bytes=24 << 20)
    partial, message = pl.pallas_call(
        local_filter_kernel,
        out_shape=(pltpu.VMEM(correlation.shape, f32), pltpu.VMEM((4 * owners + shots, width), f32)),
        in_specs=[hbm, hbm, hbm],
        out_specs=(vmem, vmem),
        scratch_shapes=[
            pltpu.VMEM((shots, rows + 2, cols, slab), f32),
            pltpu.VMEM(correlation.shape, f32),
            pltpu.VMEM(correlation.shape, f32),
            pltpu.SMEM(aperture.shape, aperture.dtype),
            pltpu.SemaphoreType.DMA((2, shots)),
            pltpu.SemaphoreType.DMA,
        ],
        compiler_params=params,
        name="local_filter",
    )(in_hbm(aperture), in_hbm(correlation), in_hbm(illumination))
    messages = [message]
    for k in range(1, slabs):
        messages.append(lax.ppermute(message, "depth", [(i, i ^ k) for i in range(slabs)]))
    place = jnp.stack([lax.axis_index("shot"), lax.axis_index("depth")])

    def finish_body(aperture, place, partial, *refs):
        finish_filter_kernel(aperture, place, partial, refs[:slabs], refs[slabs : slabs + owners], *refs[slabs + owners :])

    block = pltpu.VMEM((shots * own * (cols // 2 + 2) + 2 * shots, slab), f32)
    blocks = list(pl.pallas_call(
        finish_body,
        out_shape=(block,) * owners,
        in_specs=[smem, smem] + [vmem] * (1 + slabs),
        out_specs=(vmem,) * owners,
        scratch_shapes=[
            pltpu.VMEM((slabs,) + message.shape, f32),
            pltpu.VMEM((owners, shots * own, cols, slab), f32),
        ],
        compiler_params=params,
        name="finish_filter",
    )(aperture, place, *(in_vmem(v) for v in (partial, *messages))))
    for k in range(1, owners):
        blocks[k] = lax.ppermute(blocks[k], "shot", [(i, i ^ k) for i in range(owners)])
    cells = rows * cols * slab * slabs

    def combine_body(*refs):
        combine_kernel(cells, shots * owners, shots, refs[:owners], *refs[owners:])

    return pl.pallas_call(
        combine_body,
        out_shape=jax.ShapeDtypeStruct((own, cols, slab), f32),
        in_specs=[vmem] * owners,
        out_specs=vmem,
        scratch_shapes=[pltpu.VMEM((owners * shots, slab), f32)],
        compiler_params=params,
        name="combine",
    )(*(in_vmem(v) for v in blocks))


def solution(mesh):
    return jax.shard_map(
        on_device,
        mesh=mesh,
        in_specs=(P("shot", None, None, "depth"), P("shot", None, None, "depth"), P("shot", None)),
        out_specs=P("shot", None, "depth"),
        check_vma=False,
    )
```

```python
import math

import jax
import jax.numpy as jnp
from jax import lax
from jax.experimental import pallas as pl
from jax.experimental.pallas import tpu as pltpu
from jax.sharding import PartitionSpec as P


def local_filter_kernel(
    aperture_hbm, correlation_hbm, illumination_hbm, place_hbm, partial, message, handed,
    padded, correlation, illumination, aperture, place, arrived, read,
):
    shots, rows, cols, slab = correlation.shape
    own = message.shape[1] // (shots * cols)
    owners = rows // own
    boxes = pltpu.make_async_copy(aperture_hbm, aperture, read.at[0])
    boxes.start()
    where = pltpu.make_async_copy(place_hbm, place, read.at[1])
    where.start()
    copies = []
    for s in range(shots):
        copies.append((
            pltpu.make_async_copy(correlation_hbm.at[s], correlation.at[s], arrived.at[0, s]),
            pltpu.make_async_copy(illumination_hbm.at[s], illumination.at[s], arrived.at[1, s]),
        ))
        for copy in copies[s]:
            copy.start()
    second = lax.broadcasted_iota(jnp.int32, (cols, slab), 0)
    lane = lax.broadcasted_iota(jnp.int32, (cols, slab), 1)
    zero = jnp.zeros((cols, slab), jnp.float32)
    boxes.wait()
    for s in range(shots):
        padded[s, 0] = zero
        padded[s, rows + 1] = zero
        for copy in copies[s]:
            copy.wait()
        in_cols = (second >= aperture[s, 2]) & (second < aperture[s, 3])
        for x in range(rows):
            keep = in_cols & (x >= aperture[s, 0]) & (x < aperture[s, 1])
            padded[s, x + 1] = jnp.where(keep, correlation[s, x] / (illumination[s, x] + 0.1), 0.0)
        total = zero
        for x in range(rows):
            n = padded[s, x + 1]
            beside = padded[s, x] + padded[s, x + 2]
            beside += jnp.where(second == 0, 0.0, pltpu.roll(n, 1, 0))
            beside += jnp.where(second == cols - 1, 0.0, pltpu.roll(n, cols - 1, 0))
            beside += jnp.where(lane == 0, 0.0, pltpu.roll(n, 1, 1))
            beside += jnp.where(lane == slab - 1, 0.0, pltpu.roll(n, slab - 1, 1))
            value = 6.0 * n - beside
            partial[s, x] = value
            total += value * value
        message[4 * owners + s : 4 * owners + s + 1] = jnp.sum(total, axis=0, keepdims=True)
    for r in range(owners):
        for at, image, shift in ((0, padded, 1), (2 * owners, partial, 0)):
            held = [image[s, r * own + j + shift] for s in range(shots) for j in range(own)]
            turned = jnp.concatenate(held, axis=0).T
            message[at + r : at + r + 1] = turned[0:1]
            message[at + owners + r : at + owners + r + 1] = turned[slab - 1 : slab]
    edges = 4 * owners + shots
    handed[0:edges] = message[...]
    window = cols // 2 + 2
    where.wait()
    partner_first = (1 - place[1] % 2) * (owners // 2)
    for k in range(owners // 2):
        r = place[0] ^ (partner_first + k)
        for s in range(shots):
            for j in range(own):
                at = edges + (k * shots * own + s * own + j) * window
                handed[at : at + window] = partial[s, r * own + j, pl.ds(window_start(aperture, s, cols), window)]


def window_start(aperture, s, cols):
    return jnp.clip(aperture[s, 2] - 1, 0, cols // 2 - 2)


def finish_filter_kernel(aperture, place, partial, handed, messages, blocks, slabs_held, halo):
    shots, rows, cols, slab = partial.shape
    slabs = len(messages)
    edges, width = messages[0].shape
    own = width // (shots * cols)
    owners = rows // own
    window = cols // 2 + 2
    here = place[1]
    for k in range(slabs):
        slabs_held[here ^ k] = messages[k][...] if k != 1 else handed[0:edges]
    cross = jnp.zeros((owners, width), jnp.float32)
    for d in range(slabs - 1):
        right = slabs_held[d + 1, 0:owners]
        left = slabs_held[d, owners : 2 * owners]
        cross += right * (right - 2.0 * slabs_held[d, 3 * owners : 4 * owners])
        cross += left * (left - 2.0 * slabs_held[d + 1, 2 * owners : 3 * owners])
    cross = jnp.sum(cross, axis=0, keepdims=True)
    lane = lax.broadcasted_iota(jnp.int32, (1, width), 1)
    starts = [window_start(aperture, s, cols) for s in range(shots)]
    tails = []
    for s in range(shots):
        energy = jnp.where((lane >= s * own * cols) & (lane < (s + 1) * own * cols), cross, 0.0)
        for d in range(slabs):
            energy += slabs_held[d, 4 * owners + s : 4 * owners + s + 1]
        tails.append(energy)
    tails += [jnp.full((1, width), start.astype(jnp.float32)) for start in starts]
    tail = jnp.concatenate(tails, axis=0)
    depth = lax.broadcasted_iota(jnp.int32, (slab, width), 0)
    first = (here % 2) * (owners // 2)
    for whose in range(2):
        d = here ^ whose
        below = jnp.maximum(d - 1, 0)
        above = jnp.minimum(d + 1, slabs - 1)
        has_below = (depth == 0) & (d > 0)
        has_above = (depth == slab - 1) & (d < slabs - 1)
        for k in range(owners // 2):
            r = place[0] ^ (first + k)
            low = slabs_held[below, pl.ds(owners + r, 1)]
            high = slabs_held[above, pl.ds(r, 1)]
            halo[whose, k] = jnp.where(has_below, low, jnp.where(has_above, high, 0.0)).T
            for s in range(shots):
                for j in range(own):
                    i = s * own + j
                    if whose:
                        at = edges + (k * shots * own + i) * window
                        value = handed[at : at + window]
                    else:
                        value = partial[s, r * own + j, pl.ds(starts[s], window)]
                    blocks[k][whose, i * window : (i + 1) * window] = value - halo[whose, k, pl.ds(i * cols + starts[s], window)]
            blocks[k][whose, shots * own * window :] = tail


def combine_kernel(cells, total_shots, shots, blocks, stack, weights):
    owners = len(blocks)
    own, cols, slab = stack.shape
    window = cols // 2 + 2
    tail = shots * own * window
    energy = jnp.concatenate([block[tail : tail + shots] for block in blocks], axis=0)
    meansq = jnp.sum(energy, axis=1, keepdims=True) / cells
    peak = jnp.max(meansq, axis=0, keepdims=True)
    weight = (1.0 / math.sqrt(total_shots)) / jnp.sqrt(meansq + 0.5 * peak + 1.0)
    weights[...] = jnp.broadcast_to(weight, (owners * shots, slab))
    stack[...] = jnp.zeros(stack.shape, jnp.float32)
    for k in range(owners):
        for s in range(shots):
            start = jnp.max(blocks[k][tail + shots + s : tail + shots + s + 1]).astype(jnp.int32)
            scale = weights[k * shots + s : k * shots + s + 1]
            for j in range(own):
                i = s * own + j
                stack[j, pl.ds(start, window)] += scale * blocks[k][i * window : (i + 1) * window]


def in_hbm(array):
    return pltpu.with_memory_space_constraint(array, pltpu.HBM)


def in_vmem(array):
    return pltpu.with_memory_space_constraint(array, pltpu.VMEM)


def on_device(correlation, illumination, aperture):
    shots, rows, cols, slab = correlation.shape
    owners, slabs = lax.axis_size("shot"), lax.axis_size("depth")
    assert owners & (owners - 1) == 0 and slabs & (slabs - 1) == 0 and rows % owners == 0
    own = rows // owners
    width = shots * own * cols
    assert width == slab == 128
    f32 = jnp.float32
    vmem = pl.BlockSpec(memory_space=pltpu.VMEM)
    hbm = pl.BlockSpec(memory_space=pltpu.HBM)
    smem = pl.BlockSpec(memory_space=pltpu.SMEM)
    params = pltpu.CompilerParams(vmem_limit_bytes=24 << 20)
    half = owners // 2
    edges, window = 4 * owners + shots, cols // 2 + 2
    sent = shots * own * window
    place = jnp.stack([lax.axis_index("shot"), lax.axis_index("depth")])
    partial, message, handed = pl.pallas_call(
        local_filter_kernel,
        out_shape=(
            pltpu.VMEM(correlation.shape, f32),
            pltpu.VMEM((edges, width), f32),
            pltpu.VMEM((edges + half * sent, width), f32),
        ),
        in_specs=[hbm, hbm, hbm, hbm],
        out_specs=(vmem, vmem, vmem),
        scratch_shapes=[
            pltpu.VMEM((shots, rows + 2, cols, slab), f32),
            pltpu.VMEM(correlation.shape, f32),
            pltpu.VMEM(correlation.shape, f32),
            pltpu.SMEM(aperture.shape, aperture.dtype),
            pltpu.SMEM(place.shape, place.dtype),
            pltpu.SemaphoreType.DMA((2, shots)),
            pltpu.SemaphoreType.DMA((2,)),
        ],
        compiler_params=params,
        name="local_filter",
    )(in_hbm(aperture), in_hbm(correlation), in_hbm(illumination), place)
    messages = [message]
    for k in range(1, slabs):
        pairs = [(i, i ^ k) for i in range(slabs)]
        if k == 1:
            handed = lax.ppermute(handed, "depth", pairs)
            messages.append(message)
        else:
            messages.append(lax.ppermute(message, "depth", pairs))

    def finish_body(aperture, place, partial, handed, *refs):
        finish_filter_kernel(
            aperture, place, partial, handed, (refs[0], None) + refs[1 : slabs - 1], refs[slabs - 1 : slabs - 1 + half], *refs[slabs - 1 + half :]
        )

    blocks = list(pl.pallas_call(
        finish_body,
        out_shape=(pltpu.VMEM((2, sent + 2 * shots, slab), f32),) * half,
        in_specs=[smem, smem] + [vmem] * (1 + slabs),
        out_specs=(vmem,) * half,
        scratch_shapes=[
            pltpu.VMEM((slabs,) + message.shape, f32),
            pltpu.VMEM((2, half, width, slab), f32),
        ],
        compiler_params=params,
        name="finish_filter",
    )(aperture, place, *(in_vmem(v) for v in (partial, handed, messages[0], *messages[2:]))))
    passed = []
    for k in range(half):
        pairs = []
        for g in range(owners):
            for d in range(slabs):
                pairs.append((g * slabs + d, (g ^ (d % 2 * half + k)) * slabs + d))
        blocks[k] = lax.ppermute(blocks[k], ("shot", "depth"), pairs)
        passed.append(lax.ppermute(blocks[k], "depth", [(i, i ^ 1) for i in range(slabs)]))
    cells = rows * cols * slab * slabs

    def combine_body(*refs):
        received = [ref.at[0] for ref in refs[:half]] + [ref.at[1] for ref in refs[half:owners]]
        combine_kernel(cells, shots * owners, shots, received, *refs[owners:])

    return pl.pallas_call(
        combine_body,
        out_shape=jax.ShapeDtypeStruct((own, cols, slab), f32),
        in_specs=[vmem] * owners,
        out_specs=vmem,
        scratch_shapes=[pltpu.VMEM((owners * shots, slab), f32)],
        compiler_params=params,
        name="combine",
    )(*(in_vmem(v) for v in blocks + passed))


def solution(mesh):
    return jax.shard_map(
        on_device,
        mesh=mesh,
        in_specs=(P("shot", None, None, "depth"), P("shot", None, None, "depth"), P("shot", None)),
        out_specs=P("shot", None, "depth"),
        check_vma=False,
    )
```

```python
import math

import jax
import jax.numpy as jnp
from jax import lax
from jax.experimental import pallas as pl
from jax.experimental.pallas import tpu as pltpu
from jax.sharding import PartitionSpec as P


def partner_of(here, core, k):
    return here ^ (2 * k + core)


def local_filter_kernel(
    aperture_hbm, correlation_hbm, illumination_hbm, partial, message, handed, early,
    padded, correlation, illumination, aperture, arrived, read,
):
    shots, rows, cols, slab = correlation.shape
    own = message.shape[1] // (shots * cols)
    owners = rows // own
    window = cols // 2 + 2
    boxes = pltpu.make_async_copy(aperture_hbm, aperture, read)
    boxes.start()
    copies = []
    for s in range(shots):
        copies.append((
            pltpu.make_async_copy(correlation_hbm.at[s], correlation.at[s], arrived.at[0, s]),
            pltpu.make_async_copy(illumination_hbm.at[s], illumination.at[s], arrived.at[1, s]),
        ))
        for copy in copies[s]:
            copy.start()
    second = lax.broadcasted_iota(jnp.int32, (cols, slab), 0)
    lane = lax.broadcasted_iota(jnp.int32, (cols, slab), 1)
    zero = jnp.zeros((cols, slab), jnp.float32)
    boxes.wait()
    starts = [jnp.clip(aperture[s, 2] - 1, 0, cols - window) for s in range(shots)]
    for s in range(shots):
        padded[s, 0] = zero
        padded[s, rows + 1] = zero
        for copy in copies[s]:
            copy.wait()
        in_cols = (second >= aperture[s, 2]) & (second < aperture[s, 3])
        for x in range(rows):
            keep = in_cols & (x >= aperture[s, 0]) & (x < aperture[s, 1])
            padded[s, x + 1] = jnp.where(keep, correlation[s, x] / (illumination[s, x] + 0.1), 0.0)
        total = zero
        for x in range(rows):
            n = padded[s, x + 1]
            beside = padded[s, x] + padded[s, x + 2]
            beside += jnp.where(second == 0, 0.0, pltpu.roll(n, 1, 0))
            beside += jnp.where(second == cols - 1, 0.0, pltpu.roll(n, cols - 1, 0))
            beside += jnp.where(lane == 0, 0.0, pltpu.roll(n, 1, 1))
            beside += jnp.where(lane == slab - 1, 0.0, pltpu.roll(n, slab - 1, 1))
            value = 6.0 * n - beside
            partial[s, x] = value
            total += value * value
        message[4 * owners + s : 4 * owners + s + 1] = jnp.sum(total, axis=0, keepdims=True)
        at = 4 * owners + shots + s
        message[at : at + 1] = jnp.full((1, slab), starts[s].astype(jnp.float32))
    for r in range(owners):
        for at, image, shift in ((0, padded, 1), (2 * owners, partial, 0)):
            held = [image[s, r * own + j + shift] for s in range(shots) for j in range(own)]
            turned = jnp.concatenate(held, axis=0).T
            message[at + r : at + r + 1] = turned[0:1]
            message[at + owners + r : at + owners + r + 1] = turned[slab - 1 : slab]
    edges = message.shape[0]
    handed[0:edges] = message[...]
    mine, core = lax.axis_index("shot"), lax.axis_index("depth") % 2
    for k in range(owners // 2):
        r = partner_of(mine, 1 - core, k)
        for s in range(shots):
            for j in range(own):
                at = edges + (k * shots * own + s * own + j) * window
                handed[at : at + window] = partial[s, r * own + j, pl.ds(starts[s], window)]
    r = partner_of(mine, core, owners // 2 - 1)
    for s in range(shots):
        for j in range(own):
            at = (s * own + j) * window
            early[at : at + window] = partial[s, r * own + j, pl.ds(starts[s], window)]


def finish_filter_kernel(partial, handed, messages, blocks, slabs_held, halo):
    shots, rows, cols, slab = partial.shape
    slabs = len(messages)
    edges, width = messages[0].shape
    own = width // (shots * cols)
    owners = rows // own
    half = owners // 2
    window = cols // 2 + 2
    sent = shots * own * window
    mine, here = lax.axis_index("shot"), lax.axis_index("depth")
    for k in range(slabs):
        slabs_held[here ^ k] = messages[k][...] if k != 1 else handed[0:edges]
    cross = jnp.zeros((owners, width), jnp.float32)
    for d in range(slabs - 1):
        right = slabs_held[d + 1, 0:owners]
        left = slabs_held[d, owners : 2 * owners]
        cross += right * (right - 2.0 * slabs_held[d, 3 * owners : 4 * owners])
        cross += left * (left - 2.0 * slabs_held[d + 1, 2 * owners : 3 * owners])
    cross = jnp.sum(cross, axis=0, keepdims=True)
    lane = lax.broadcasted_iota(jnp.int32, (1, width), 1)
    tails = []
    starts = []
    for s in range(shots):
        energy = jnp.where((lane >= s * own * cols) & (lane < (s + 1) * own * cols), cross, 0.0)
        for d in range(slabs):
            energy += slabs_held[d, 4 * owners + s : 4 * owners + s + 1]
        tails.append(energy)
        starts.append(jnp.max(messages[0][4 * owners + shots + s : 4 * owners + shots + s + 1]).astype(jnp.int32))
    tails.append(messages[0][4 * owners + shots :])
    tail = jnp.concatenate(tails, axis=0)
    depth = lax.broadcasted_iota(jnp.int32, (slab, width), 0)
    for whose in range(2):
        d = here ^ whose
        below = jnp.maximum(d - 1, 0)
        above = jnp.minimum(d + 1, slabs - 1)
        for k in range(half):
            r = partner_of(mine, here % 2, k)
            low = jnp.where(d > 0, slabs_held[below, pl.ds(owners + r, 1)], 0.0)
            high = jnp.where(d < slabs - 1, slabs_held[above, pl.ds(r, 1)], 0.0)
            last = k == half - 1
            if last and not whose:
                blocks[k][0:1] = low
                blocks[k][1:2] = high
                continue
            halo[whose, k] = jnp.where(depth == 0, low, jnp.where(depth == slab - 1, high, 0.0)).T
            for s in range(shots):
                for j in range(own):
                    i = s * own + j
                    if whose:
                        at = edges + (k * shots * own + i) * window
                        value = handed[at : at + window]
                        at = (2 if last else sent) + i * window
                    else:
                        value = partial[s, r * own + j, pl.ds(starts[s], window)]
                        at = i * window
                    blocks[k][at : at + window] = value - halo[whose, k, pl.ds(i * cols + starts[s], window)]
    for k in range(half):
        blocks[k][blocks[k].shape[0] - 2 * shots :] = tail


def combine_kernel(cells, total_shots, shots, parts, early, layers, stack, weights, halo):
    own, cols, slab = stack.shape
    window = cols // 2 + 2
    tails = [block.shape[0] - 2 * shots for block, _ in parts]
    energy = jnp.concatenate([block[at : at + shots] for (block, _), at in zip(parts, tails)], axis=0)
    meansq = jnp.sum(energy, axis=1, keepdims=True) / cells
    peak = jnp.max(meansq, axis=0, keepdims=True)
    weight = (1.0 / math.sqrt(total_shots)) / jnp.sqrt(meansq + 0.5 * peak + 1.0)
    weights[...] = jnp.broadcast_to(weight, weights.shape)
    stack[...] = jnp.zeros(stack.shape, jnp.float32)
    width = shots * own * cols
    depth = lax.broadcasted_iota(jnp.int32, (slab, width), 0)
    halo[...] = jnp.where(depth == 0, layers[0:1], jnp.where(depth == slab - 1, layers[1:2], 0.0)).T
    for k, ((block, rows), tail) in enumerate(zip(parts, tails)):
        for s in range(shots):
            at = tail + shots + s
            start = jnp.max(block[at : at + 1]).astype(jnp.int32)
            scale = weights[k * shots + s : k * shots + s + 1]
            for j in range(own):
                i = s * own + j
                if rows is None:
                    value = early[i * window : (i + 1) * window] - halo[pl.ds(i * cols + start, window)]
                else:
                    value = block[rows + i * window : rows + (i + 1) * window]
                stack[j, pl.ds(start, window)] += scale * value


def in_hbm(array):
    return pltpu.with_memory_space_constraint(array, pltpu.HBM)


def in_vmem(array):
    return pltpu.with_memory_space_constraint(array, pltpu.VMEM)


def on_device(correlation, illumination, aperture):
    shots, rows, cols, slab = correlation.shape
    owners, slabs = lax.axis_size("shot"), lax.axis_size("depth")
    assert owners & (owners - 1) == 0 and slabs & (slabs - 1) == 0 and rows % owners == 0
    own = rows // owners
    width = shots * own * cols
    assert width == slab == 128
    half = owners // 2
    edges, window = 4 * owners + 2 * shots, cols // 2 + 2
    sent = shots * own * window
    f32 = jnp.float32
    vmem = pl.BlockSpec(memory_space=pltpu.VMEM)
    hbm = pl.BlockSpec(memory_space=pltpu.HBM)
    params = pltpu.CompilerParams(vmem_limit_bytes=24 << 20)
    partial, message, handed, early = pl.pallas_call(
        local_filter_kernel,
        out_shape=(
            pltpu.VMEM(correlation.shape, f32),
            pltpu.VMEM((edges, width), f32),
            pltpu.VMEM((edges + half * sent, width), f32),
            pltpu.VMEM((sent, width), f32),
        ),
        in_specs=[hbm, hbm, hbm],
        out_specs=(vmem, vmem, vmem, vmem),
        scratch_shapes=[
            pltpu.VMEM((shots, rows + 2, cols, slab), f32),
            pltpu.VMEM(correlation.shape, f32),
            pltpu.VMEM(correlation.shape, f32),
            pltpu.SMEM(aperture.shape, aperture.dtype),
            pltpu.SemaphoreType.DMA((2, shots)),
            pltpu.SemaphoreType.DMA,
        ],
        compiler_params=params,
        name="local_filter",
    )(in_hbm(aperture), in_hbm(correlation), in_hbm(illumination))

    def round_pairs(k):
        pairs = []
        for g in range(owners):
            for d in range(slabs):
                pairs.append((g * slabs + d, partner_of(g, d % 2, k) * slabs + d))
        return pairs

    messages = [message]
    for k in range(1, slabs):
        pairs = [(i, i ^ k) for i in range(slabs)]
        if k == 1:
            handed = lax.ppermute(handed, "depth", pairs)
            messages.append(message)
        else:
            messages.append(lax.ppermute(message, "depth", pairs))
    early = lax.ppermute(early, ("shot", "depth"), round_pairs(half - 1))

    def finish_body(partial, handed, *refs):
        finish_filter_kernel(
            partial, handed, (refs[0], None) + refs[1 : slabs - 1], refs[slabs - 1 : slabs - 1 + half], *refs[slabs - 1 + half :]
        )

    block = pltpu.VMEM((2 * sent + 2 * shots, slab), f32)
    light = pltpu.VMEM((2 + sent + 2 * shots, slab), f32)
    blocks = list(pl.pallas_call(
        finish_body,
        out_shape=(block,) * (half - 1) + (light,),
        in_specs=[vmem] * (1 + slabs),
        out_specs=(vmem,) * half,
        scratch_shapes=[
            pltpu.VMEM((slabs,) + message.shape, f32),
            pltpu.VMEM((2, half, width, slab), f32),
        ],
        compiler_params=params,
        name="finish_filter",
    )(*(in_vmem(v) for v in (partial, handed, messages[0], *messages[2:]))))
    passed = []
    for k in range(half):
        blocks[k] = lax.ppermute(blocks[k], ("shot", "depth"), round_pairs(k))
        passed.append(lax.ppermute(blocks[k], "depth", [(i, i ^ 1) for i in range(slabs)]))
    cells = rows * cols * slab * slabs

    def combine_body(early, *refs):
        ours, theirs = refs[:half], refs[half:owners]
        parts = [(ref, None if k == half - 1 else 0) for k, ref in enumerate(ours)]
        parts += [(ref, 2 if k == half - 1 else sent) for k, ref in enumerate(theirs)]
        combine_kernel(cells, shots * owners, shots, parts, early, ours[half - 1], *refs[owners:])

    return pl.pallas_call(
        combine_body,
        out_shape=jax.ShapeDtypeStruct((own, cols, slab), f32),
        in_specs=[vmem] * (1 + owners),
        out_specs=vmem,
        scratch_shapes=[pltpu.VMEM((owners * shots, slab), f32), pltpu.VMEM((width, slab), f32)],
        compiler_params=params,
        name="combine",
    )(*(in_vmem(v) for v in [early] + blocks + passed))


def solution(mesh):
    return jax.shard_map(
        on_device,
        mesh=mesh,
        in_specs=(P("shot", None, None, "depth"), P("shot", None, None, "depth"), P("shot", None)),
        out_specs=P("shot", None, "depth"),
        check_vma=False,
    )
```

```python
import math

import jax
import jax.numpy as jnp
from jax import lax
from jax.experimental import pallas as pl
from jax.experimental.pallas import tpu as pltpu
from jax.sharding import PartitionSpec as P


EARLY_ROUNDS = 1


def partner_of(here, core, k):
    return here ^ (2 * k + (core + k + k // 2) % 2)


def local_filter_kernel(
    aperture_hbm, correlation_hbm, illumination_hbm, partial, message, handed, early,
    padded, correlation, illumination, aperture, arrived, read,
):
    shots, rows, cols, slab = correlation.shape
    own = message.shape[1] // (shots * cols)
    owners = rows // own
    window = cols // 2 + 2
    boxes = pltpu.make_async_copy(aperture_hbm, aperture, read)
    boxes.start()
    copies = []
    for s in range(shots):
        copies.append((
            pltpu.make_async_copy(correlation_hbm.at[s], correlation.at[s], arrived.at[0, s]),
            pltpu.make_async_copy(illumination_hbm.at[s], illumination.at[s], arrived.at[1, s]),
        ))
        for copy in copies[s]:
            copy.start()
    second = lax.broadcasted_iota(jnp.int32, (cols, slab), 0)
    lane = lax.broadcasted_iota(jnp.int32, (cols, slab), 1)
    zero = jnp.zeros((cols, slab), jnp.float32)
    boxes.wait()
    starts = [jnp.clip(aperture[s, 2] - 1, 0, cols - window) for s in range(shots)]
    for s in range(shots):
        padded[s, 0] = zero
        padded[s, rows + 1] = zero
        for copy in copies[s]:
            copy.wait()
        in_cols = (second >= aperture[s, 2]) & (second < aperture[s, 3])
        for x in range(rows):
            keep = in_cols & (x >= aperture[s, 0]) & (x < aperture[s, 1])
            padded[s, x + 1] = jnp.where(keep, correlation[s, x] / (illumination[s, x] + 0.1), 0.0)
        total = zero
        for x in range(rows):
            n = padded[s, x + 1]
            beside = padded[s, x] + padded[s, x + 2]
            beside += jnp.where(second == 0, 0.0, pltpu.roll(n, 1, 0))
            beside += jnp.where(second == cols - 1, 0.0, pltpu.roll(n, cols - 1, 0))
            beside += jnp.where(lane == 0, 0.0, pltpu.roll(n, 1, 1))
            beside += jnp.where(lane == slab - 1, 0.0, pltpu.roll(n, slab - 1, 1))
            value = 6.0 * n - beside
            partial[s, x] = value
            total += value * value
        message[4 * owners + s : 4 * owners + s + 1] = jnp.sum(total, axis=0, keepdims=True)
        at = 4 * owners + shots + s
        message[at : at + 1] = jnp.full((1, slab), starts[s].astype(jnp.float32))
    for r in range(owners):
        for at, image, shift in ((0, padded, 1), (2 * owners, partial, 0)):
            held = [image[s, r * own + j + shift] for s in range(shots) for j in range(own)]
            turned = jnp.concatenate(held, axis=0).T
            message[at + r : at + r + 1] = turned[0:1]
            message[at + owners + r : at + owners + r + 1] = turned[slab - 1 : slab]
    edges = message.shape[0]
    handed[0:edges] = message[...]
    mine, core = lax.axis_index("shot"), lax.axis_index("depth") % 2
    for k in range(owners // 2):
        r = partner_of(mine, 1 - core, k)
        for s in range(shots):
            for j in range(own):
                at = edges + (k * shots * own + s * own + j) * window
                handed[at : at + window] = partial[s, r * own + j, pl.ds(starts[s], window)]
    for k, block in early.items():
        r = partner_of(mine, core, k)
        for s in range(shots):
            for j in range(own):
                at = (s * own + j) * window
                block[at : at + window] = partial[s, r * own + j, pl.ds(starts[s], window)]


def finish_filter_kernel(ahead, partial, handed, messages, blocks, slabs_held, halo):
    shots, rows, cols, slab = partial.shape
    slabs = len(messages)
    edges, width = messages[0].shape
    own = width // (shots * cols)
    owners = rows // own
    half = owners // 2
    window = cols // 2 + 2
    sent = shots * own * window
    mine, here = lax.axis_index("shot"), lax.axis_index("depth")
    for k in range(slabs):
        slabs_held[here ^ k] = messages[k][...] if k != 1 else handed[0:edges]
    cross = jnp.zeros((owners, width), jnp.float32)
    for d in range(slabs - 1):
        right = slabs_held[d + 1, 0:owners]
        left = slabs_held[d, owners : 2 * owners]
        cross += right * (right - 2.0 * slabs_held[d, 3 * owners : 4 * owners])
        cross += left * (left - 2.0 * slabs_held[d + 1, 2 * owners : 3 * owners])
    cross = jnp.sum(cross, axis=0, keepdims=True)
    lane = lax.broadcasted_iota(jnp.int32, (1, width), 1)
    tails = []
    starts = []
    for s in range(shots):
        energy = jnp.where((lane >= s * own * cols) & (lane < (s + 1) * own * cols), cross, 0.0)
        for d in range(slabs):
            energy += slabs_held[d, 4 * owners + s : 4 * owners + s + 1]
        tails.append(energy)
        starts.append(jnp.max(messages[0][4 * owners + shots + s : 4 * owners + shots + s + 1]).astype(jnp.int32))
    tails.append(messages[0][4 * owners + shots :])
    tail = jnp.concatenate(tails, axis=0)
    depth = lax.broadcasted_iota(jnp.int32, (slab, width), 0)
    for whose in range(2):
        d = here ^ whose
        below = jnp.maximum(d - 1, 0)
        above = jnp.minimum(d + 1, slabs - 1)
        for k in range(half):
            r = partner_of(mine, here % 2, k)
            low = jnp.where(d > 0, slabs_held[below, pl.ds(owners + r, 1)], 0.0)
            high = jnp.where(d < slabs - 1, slabs_held[above, pl.ds(r, 1)], 0.0)
            if k in ahead and not whose:
                blocks[k][0:1] = low
                blocks[k][1:2] = high
                continue
            halo[whose, k] = jnp.where(depth == 0, low, jnp.where(depth == slab - 1, high, 0.0)).T
            for s in range(shots):
                for j in range(own):
                    i = s * own + j
                    if whose:
                        at = edges + (k * shots * own + i) * window
                        value = handed[at : at + window]
                        at = (2 if k in ahead else sent) + i * window
                    else:
                        value = partial[s, r * own + j, pl.ds(starts[s], window)]
                        at = i * window
                    blocks[k][at : at + window] = value - halo[whose, k, pl.ds(i * cols + starts[s], window)]
    for k in range(half):
        blocks[k][blocks[k].shape[0] - 2 * shots :] = tail


def combine_kernel(cells, total_shots, shots, parts, stack, weights, halo):
    own, cols, slab = stack.shape
    window = cols // 2 + 2
    tails = [block.shape[0] - 2 * shots for block, _, _ in parts]
    energy = jnp.concatenate([part[0][at : at + shots] for part, at in zip(parts, tails)], axis=0)
    meansq = jnp.sum(energy, axis=1, keepdims=True) / cells
    peak = jnp.max(meansq, axis=0, keepdims=True)
    weight = (1.0 / math.sqrt(total_shots)) / jnp.sqrt(meansq + 0.5 * peak + 1.0)
    weights[...] = jnp.broadcast_to(weight, weights.shape)
    stack[...] = jnp.zeros(stack.shape, jnp.float32)
    depth = lax.broadcasted_iota(jnp.int32, (slab, shots * own * cols), 0)
    for k, ((block, rows, early), tail) in enumerate(zip(parts, tails)):
        if early is not None:
            halo[k] = jnp.where(depth == 0, block[0:1], jnp.where(depth == slab - 1, block[1:2], 0.0)).T
        for s in range(shots):
            at = tail + shots + s
            start = jnp.max(block[at : at + 1]).astype(jnp.int32)
            scale = weights[k * shots + s : k * shots + s + 1]
            for j in range(own):
                i = s * own + j
                if early is not None:
                    value = early[i * window : (i + 1) * window] - halo[k, pl.ds(i * cols + start, window)]
                else:
                    value = block[rows + i * window : rows + (i + 1) * window]
                stack[j, pl.ds(start, window)] += scale * value


def in_hbm(array):
    return pltpu.with_memory_space_constraint(array, pltpu.HBM)


def in_vmem(array):
    return pltpu.with_memory_space_constraint(array, pltpu.VMEM)


def on_device(correlation, illumination, aperture):
    shots, rows, cols, slab = correlation.shape
    owners, slabs = lax.axis_size("shot"), lax.axis_size("depth")
    assert owners & (owners - 1) == 0 and slabs & (slabs - 1) == 0 and rows % owners == 0
    own = rows // owners
    width = shots * own * cols
    assert width == slab == 128
    half = owners // 2
    edges, window = 4 * owners + 2 * shots, cols // 2 + 2
    sent = shots * own * window
    f32 = jnp.float32
    vmem = pl.BlockSpec(memory_space=pltpu.VMEM)
    hbm = pl.BlockSpec(memory_space=pltpu.HBM)
    params = pltpu.CompilerParams(vmem_limit_bytes=24 << 20)
    ahead = range(half - EARLY_ROUNDS, half)

    def local_body(aperture, correlation, illumination, partial, message, handed, *refs):
        early = dict(zip(ahead, refs))
        local_filter_kernel(aperture, correlation, illumination, partial, message, handed, early, *refs[len(ahead) :])

    partial, message, handed, *early = pl.pallas_call(
        local_body,
        out_shape=(
            pltpu.VMEM(correlation.shape, f32),
            pltpu.VMEM((edges, width), f32),
            pltpu.VMEM((edges + half * sent, width), f32),
            *(pltpu.VMEM((sent, width), f32) for _ in ahead),
        ),
        in_specs=[hbm, hbm, hbm],
        out_specs=(vmem,) * (3 + len(ahead)),
        scratch_shapes=[
            pltpu.VMEM((shots, rows + 2, cols, slab), f32),
            pltpu.VMEM(correlation.shape, f32),
            pltpu.VMEM(correlation.shape, f32),
            pltpu.SMEM(aperture.shape, aperture.dtype),
            pltpu.SemaphoreType.DMA((2, shots)),
            pltpu.SemaphoreType.DMA,
        ],
        compiler_params=params,
        name="local_filter",
    )(in_hbm(aperture), in_hbm(correlation), in_hbm(illumination))

    def round_pairs(k):
        pairs = []
        for g in range(owners):
            for d in range(slabs):
                pairs.append((g * slabs + d, partner_of(g, d % 2, k) * slabs + d))
        return pairs

    messages = [message]
    for k in range(1, slabs):
        pairs = [(i, i ^ k) for i in range(slabs)]
        if k == 1:
            handed = lax.ppermute(handed, "depth", pairs)
            messages.append(message)
        else:
            messages.append(lax.ppermute(message, "depth", pairs))
    for at, k in enumerate(ahead):
        early[at] = lax.ppermute(early[at], ("shot", "depth"), round_pairs(k))

    def finish_body(partial, handed, *refs):
        finish_filter_kernel(
            ahead, partial, handed, (refs[0], None) + refs[1 : slabs - 1], refs[slabs - 1 : slabs - 1 + half], *refs[slabs - 1 + half :]
        )

    block = pltpu.VMEM((2 * sent + 2 * shots, slab), f32)
    light = pltpu.VMEM((2 + sent + 2 * shots, slab), f32)
    blocks = list(pl.pallas_call(
        finish_body,
        out_shape=(block,) * (half - len(ahead)) + (light,) * len(ahead),
        in_specs=[vmem] * (1 + slabs),
        out_specs=(vmem,) * half,
        scratch_shapes=[
            pltpu.VMEM((slabs,) + message.shape, f32),
            pltpu.VMEM((2, half, width, slab), f32),
        ],
        compiler_params=params,
        name="finish_filter",
    )(*(in_vmem(v) for v in (partial, handed, messages[0], *messages[2:]))))
    passed = []
    for k in range(half):
        blocks[k] = lax.ppermute(blocks[k], ("shot", "depth"), round_pairs(k))
        passed.append(lax.ppermute(blocks[k], "depth", [(i, i ^ 1) for i in range(slabs)]))
    cells = rows * cols * slab * slabs

    def combine_body(*refs):
        early = dict(zip(ahead, refs))
        ours, theirs, rest = (refs[len(ahead) + at :] for at in (0, half, owners))
        parts = [(ours[k], 0, early.get(k)) for k in range(half)]
        parts += [(theirs[k], 2 if k in early else sent, None) for k in range(half)]
        combine_kernel(cells, shots * owners, shots, parts, *rest)

    return pl.pallas_call(
        combine_body,
        out_shape=jax.ShapeDtypeStruct((own, cols, slab), f32),
        in_specs=[vmem] * (len(ahead) + owners),
        out_specs=vmem,
        scratch_shapes=[pltpu.VMEM((owners * shots, slab), f32), pltpu.VMEM((half, width, slab), f32)],
        compiler_params=params,
        name="combine",
    )(*(in_vmem(v) for v in early + blocks + passed))


def solution(mesh):
    return jax.shard_map(
        on_device,
        mesh=mesh,
        in_specs=(P("shot", None, None, "depth"), P("shot", None, None, "depth"), P("shot", None)),
        out_specs=P("shot", None, "depth"),
        check_vma=False,
    )
```

```python
import math

import jax
import jax.numpy as jnp
from jax import lax
from jax.experimental import pallas as pl
from jax.experimental.pallas import tpu as pltpu
from jax.sharding import PartitionSpec as P


EARLY_ROUNDS = 1


def partner_of(here, core, k):
    return here ^ (2 * k + (core + k + k // 2) % 2)


def local_filter_kernel(
    aperture_hbm, correlation_hbm, illumination_hbm, partial, message, handed, early,
    padded, correlation, illumination, aperture, arrived, read,
):
    shots, rows, cols, slab = correlation.shape
    own = message.shape[1] // (shots * cols)
    owners = rows // own
    window = cols // 2 + 2
    boxes = pltpu.make_async_copy(aperture_hbm, aperture, read)
    boxes.start()
    copies = []
    for s in range(shots):
        copies.append((
            pltpu.make_async_copy(correlation_hbm.at[s], correlation.at[s], arrived.at[0, s]),
            pltpu.make_async_copy(illumination_hbm.at[s], illumination.at[s], arrived.at[1, s]),
        ))
        for copy in copies[s]:
            copy.start()
    second = lax.broadcasted_iota(jnp.int32, (cols, slab), 0)
    lane = lax.broadcasted_iota(jnp.int32, (cols, slab), 1)
    zero = jnp.zeros((cols, slab), jnp.float32)
    rim = jnp.zeros((cols + 16, slab), jnp.float32)
    boxes.wait()
    starts = [jnp.clip(aperture[s, 2] - 1, 0, cols - window) for s in range(shots)]
    for s in range(shots):
        padded[s, 0] = rim
        padded[s, rows + 1] = rim
        for x in range(rows):
            padded[s, x + 1, 0:8] = rim[0:8]
            padded[s, x + 1, cols + 8 : cols + 16] = rim[0:8]
        for copy in copies[s]:
            copy.wait()
        in_cols = (second >= aperture[s, 2]) & (second < aperture[s, 3])
        for x in range(rows):
            keep = in_cols & (x >= aperture[s, 0]) & (x < aperture[s, 1])
            padded[s, x + 1, 8 : cols + 8] = jnp.where(keep, correlation[s, x] / (illumination[s, x] + 0.1), 0.0)
        total = zero
        for x in range(rows):
            n = padded[s, x + 1, 8 : cols + 8]
            beside = padded[s, x, 8 : cols + 8] + padded[s, x + 2, 8 : cols + 8]
            beside += padded[s, x + 1, 7 : cols + 7] + padded[s, x + 1, 9 : cols + 9]
            beside += jnp.where(lane == 0, 0.0, pltpu.roll(n, 1, 1))
            beside += jnp.where(lane == slab - 1, 0.0, pltpu.roll(n, slab - 1, 1))
            value = 6.0 * n - beside
            partial[s, x] = value
            total += value * value
        message[4 * owners + s : 4 * owners + s + 1] = jnp.sum(total, axis=0, keepdims=True)
        at = 4 * owners + shots + s
        message[at : at + 1] = jnp.full((1, slab), starts[s].astype(jnp.float32))
    for r in range(owners):
        for at, image, shift, top in ((0, padded, 1, 8), (2 * owners, partial, 0, 0)):
            held = [image[s, r * own + j + shift, top : top + cols] for s in range(shots) for j in range(own)]
            turned = jnp.concatenate(held, axis=0).T
            message[at + r : at + r + 1] = turned[0:1]
            message[at + owners + r : at + owners + r + 1] = turned[slab - 1 : slab]
    edges = message.shape[0]
    handed[0:edges] = message[...]
    mine, core = lax.axis_index("shot"), lax.axis_index("depth") % 2
    for k in range(owners // 2):
        r = partner_of(mine, 1 - core, k)
        for s in range(shots):
            for j in range(own):
                at = edges + (k * shots * own + s * own + j) * window
                handed[at : at + window] = partial[s, r * own + j, pl.ds(starts[s], window)]
    for k, block in early.items():
        r = partner_of(mine, core, k)
        for s in range(shots):
            for j in range(own):
                at = (s * own + j) * window
                block[at : at + window] = partial[s, r * own + j, pl.ds(starts[s], window)]


def finish_filter_kernel(ahead, partial, handed, messages, blocks, slabs_held, halo):
    shots, rows, cols, slab = partial.shape
    slabs = len(messages)
    edges, width = messages[0].shape
    own = width // (shots * cols)
    owners = rows // own
    half = owners // 2
    window = cols // 2 + 2
    sent = shots * own * window
    mine, here = lax.axis_index("shot"), lax.axis_index("depth")
    for k in range(slabs):
        slabs_held[here ^ k] = messages[k][...] if k != 1 else handed[0:edges]
    cross = jnp.zeros((owners, width), jnp.float32)
    for d in range(slabs - 1):
        right = slabs_held[d + 1, 0:owners]
        left = slabs_held[d, owners : 2 * owners]
        cross += right * (right - 2.0 * slabs_held[d, 3 * owners : 4 * owners])
        cross += left * (left - 2.0 * slabs_held[d + 1, 2 * owners : 3 * owners])
    cross = jnp.sum(cross, axis=0, keepdims=True)
    lane = lax.broadcasted_iota(jnp.int32, (1, width), 1)
    tails = []
    starts = []
    for s in range(shots):
        energy = jnp.where((lane >= s * own * cols) & (lane < (s + 1) * own * cols), cross, 0.0)
        for d in range(slabs):
            energy += slabs_held[d, 4 * owners + s : 4 * owners + s + 1]
        tails.append(energy)
        starts.append(jnp.max(messages[0][4 * owners + shots + s : 4 * owners + shots + s + 1]).astype(jnp.int32))
    tails.append(messages[0][4 * owners + shots :])
    tail = jnp.concatenate(tails, axis=0)
    depth = lax.broadcasted_iota(jnp.int32, (slab, width), 0)
    for whose in range(2):
        d = here ^ whose
        below = jnp.maximum(d - 1, 0)
        above = jnp.minimum(d + 1, slabs - 1)
        for k in range(half):
            r = partner_of(mine, here % 2, k)
            low = jnp.where(d > 0, slabs_held[below, pl.ds(owners + r, 1)], 0.0)
            high = jnp.where(d < slabs - 1, slabs_held[above, pl.ds(r, 1)], 0.0)
            if k in ahead and not whose:
                blocks[k][0:1] = low
                blocks[k][1:2] = high
                continue
            halo[whose, k] = jnp.where(depth == 0, low, jnp.where(depth == slab - 1, high, 0.0)).T
            for s in range(shots):
                for j in range(own):
                    i = s * own + j
                    if whose:
                        at = edges + (k * shots * own + i) * window
                        value = handed[at : at + window]
                        at = (2 if k in ahead else sent) + i * window
                    else:
                        value = partial[s, r * own + j, pl.ds(starts[s], window)]
                        at = i * window
                    blocks[k][at : at + window] = value - halo[whose, k, pl.ds(i * cols + starts[s], window)]
    for k in range(half):
        blocks[k][blocks[k].shape[0] - 2 * shots :] = tail


def combine_kernel(cells, total_shots, shots, parts, stack, weights, halo):
    own, cols, slab = stack.shape
    window = cols // 2 + 2
    tails = [block.shape[0] - 2 * shots for block, _, _ in parts]
    energy = jnp.concatenate([part[0][at : at + shots] for part, at in zip(parts, tails)], axis=0)
    meansq = jnp.sum(energy, axis=1, keepdims=True) / cells
    peak = jnp.max(meansq, axis=0, keepdims=True)
    weight = (1.0 / math.sqrt(total_shots)) / jnp.sqrt(meansq + 0.5 * peak + 1.0)
    weights[...] = jnp.broadcast_to(weight, weights.shape)
    stack[...] = jnp.zeros(stack.shape, jnp.float32)
    depth = lax.broadcasted_iota(jnp.int32, (slab, shots * own * cols), 0)
    for k, ((block, rows, early), tail) in enumerate(zip(parts, tails)):
        if early is not None:
            halo[k] = jnp.where(depth == 0, block[0:1], jnp.where(depth == slab - 1, block[1:2], 0.0)).T
        for s in range(shots):
            at = tail + shots + s
            start = jnp.max(block[at : at + 1]).astype(jnp.int32)
            scale = weights[k * shots + s : k * shots + s + 1]
            for j in range(own):
                i = s * own + j
                if early is not None:
                    value = early[i * window : (i + 1) * window] - halo[k, pl.ds(i * cols + start, window)]
                else:
                    value = block[rows + i * window : rows + (i + 1) * window]
                stack[j, pl.ds(start, window)] += scale * value


def in_hbm(array):
    return pltpu.with_memory_space_constraint(array, pltpu.HBM)


def in_vmem(array):
    return pltpu.with_memory_space_constraint(array, pltpu.VMEM)


def on_device(correlation, illumination, aperture):
    shots, rows, cols, slab = correlation.shape
    owners, slabs = lax.axis_size("shot"), lax.axis_size("depth")
    assert owners & (owners - 1) == 0 and slabs & (slabs - 1) == 0 and rows % owners == 0
    own = rows // owners
    width = shots * own * cols
    assert width == slab == 128
    half = owners // 2
    edges, window = 4 * owners + 2 * shots, cols // 2 + 2
    sent = shots * own * window
    f32 = jnp.float32
    vmem = pl.BlockSpec(memory_space=pltpu.VMEM)
    hbm = pl.BlockSpec(memory_space=pltpu.HBM)
    params = pltpu.CompilerParams(vmem_limit_bytes=24 << 20)
    ahead = range(half - EARLY_ROUNDS, half)

    def local_body(aperture, correlation, illumination, partial, message, handed, *refs):
        early = dict(zip(ahead, refs))
        local_filter_kernel(aperture, correlation, illumination, partial, message, handed, early, *refs[len(ahead) :])

    partial, message, handed, *early = pl.pallas_call(
        local_body,
        out_shape=(
            pltpu.VMEM(correlation.shape, f32),
            pltpu.VMEM((edges, width), f32),
            pltpu.VMEM((edges + half * sent, width), f32),
            *(pltpu.VMEM((sent, width), f32) for _ in ahead),
        ),
        in_specs=[hbm, hbm, hbm],
        out_specs=(vmem,) * (3 + len(ahead)),
        scratch_shapes=[
            pltpu.VMEM((shots, rows + 2, cols + 16, slab), f32),
            pltpu.VMEM(correlation.shape, f32),
            pltpu.VMEM(correlation.shape, f32),
            pltpu.SMEM(aperture.shape, aperture.dtype),
            pltpu.SemaphoreType.DMA((2, shots)),
            pltpu.SemaphoreType.DMA,
        ],
        compiler_params=params,
        name="local_filter",
    )(in_hbm(aperture), in_hbm(correlation), in_hbm(illumination))

    def round_pairs(k):
        pairs = []
        for g in range(owners):
            for d in range(slabs):
                pairs.append((g * slabs + d, partner_of(g, d % 2, k) * slabs + d))
        return pairs

    messages = [message]
    for k in range(1, slabs):
        pairs = [(i, i ^ k) for i in range(slabs)]
        if k == 1:
            handed = lax.ppermute(handed, "depth", pairs)
            messages.append(message)
        else:
            messages.append(lax.ppermute(message, "depth", pairs))
    for at, k in enumerate(ahead):
        early[at] = lax.ppermute(early[at], ("shot", "depth"), round_pairs(k))

    def finish_body(partial, handed, *refs):
        finish_filter_kernel(
            ahead, partial, handed, (refs[0], None) + refs[1 : slabs - 1], refs[slabs - 1 : slabs - 1 + half], *refs[slabs - 1 + half :]
        )

    block = pltpu.VMEM((2 * sent + 2 * shots, slab), f32)
    light = pltpu.VMEM((2 + sent + 2 * shots, slab), f32)
    blocks = list(pl.pallas_call(
        finish_body,
        out_shape=(block,) * (half - len(ahead)) + (light,) * len(ahead),
        in_specs=[vmem] * (1 + slabs),
        out_specs=(vmem,) * half,
        scratch_shapes=[
            pltpu.VMEM((slabs,) + message.shape, f32),
            pltpu.VMEM((2, half, width, slab), f32),
        ],
        compiler_params=params,
        name="finish_filter",
    )(*(in_vmem(v) for v in (partial, handed, messages[0], *messages[2:]))))
    passed = []
    for k in range(half):
        blocks[k] = lax.ppermute(blocks[k], ("shot", "depth"), round_pairs(k))
        passed.append(lax.ppermute(blocks[k], "depth", [(i, i ^ 1) for i in range(slabs)]))
    cells = rows * cols * slab * slabs

    def combine_body(*refs):
        early = dict(zip(ahead, refs))
        ours, theirs, rest = (refs[len(ahead) + at :] for at in (0, half, owners))
        parts = [(ours[k], 0, early.get(k)) for k in range(half)]
        parts += [(theirs[k], 2 if k in early else sent, None) for k in range(half)]
        combine_kernel(cells, shots * owners, shots, parts, *rest)

    return pl.pallas_call(
        combine_body,
        out_shape=jax.ShapeDtypeStruct((own, cols, slab), f32),
        in_specs=[vmem] * (len(ahead) + owners),
        out_specs=vmem,
        scratch_shapes=[pltpu.VMEM((owners * shots, slab), f32), pltpu.VMEM((half, width, slab), f32)],
        compiler_params=params,
        name="combine",
    )(*(in_vmem(v) for v in early + blocks + passed))


def solution(mesh):
    return jax.shard_map(
        on_device,
        mesh=mesh,
        in_specs=(P("shot", None, None, "depth"), P("shot", None, None, "depth"), P("shot", None)),
        out_specs=P("shot", None, "depth"),
        check_vma=False,
    )
```

```python
import math

import jax
import jax.numpy as jnp
from jax import lax
from jax.experimental import pallas as pl
from jax.experimental.pallas import tpu as pltpu
from jax.sharding import PartitionSpec as P


def partner_of(here, core, k):
    return here ^ (2 * k + (core + k + k // 2) % 2)


def local_filter_kernel(
    aperture_hbm, correlation_hbm, illumination_hbm, partial, message, handed, early,
    padded, correlation, illumination, aperture, arrived, read,
):
    shots, rows, cols, slab = correlation.shape
    own = message.shape[1] // (shots * cols)
    owners = rows // own
    window = cols // 2 + 2
    boxes = pltpu.make_async_copy(aperture_hbm, aperture, read)
    boxes.start()
    copies = []
    for s in range(shots):
        copies.append((
            pltpu.make_async_copy(correlation_hbm.at[s], correlation.at[s], arrived.at[0, s]),
            pltpu.make_async_copy(illumination_hbm.at[s], illumination.at[s], arrived.at[1, s]),
        ))
        for copy in copies[s]:
            copy.start()
    second = lax.broadcasted_iota(jnp.int32, (cols, slab), 0)
    lane = lax.broadcasted_iota(jnp.int32, (cols, slab), 1)
    zero = jnp.zeros((cols, slab), jnp.float32)
    rim = jnp.zeros((cols + 16, slab), jnp.float32)
    boxes.wait()
    starts = [jnp.clip(aperture[s, 2] - 1, 0, cols - window) for s in range(shots)]
    for s in range(shots):
        padded[s, 0] = rim
        padded[s, rows + 1] = rim
        for x in range(rows):
            padded[s, x + 1, 0:8] = rim[0:8]
            padded[s, x + 1, cols + 8 : cols + 16] = rim[0:8]
        for copy in copies[s]:
            copy.wait()
        in_cols = (second >= aperture[s, 2]) & (second < aperture[s, 3])
        for x in range(rows):
            keep = in_cols & (x >= aperture[s, 0]) & (x < aperture[s, 1])
            padded[s, x + 1, 8 : cols + 8] = jnp.where(keep, correlation[s, x] / (illumination[s, x] + 0.1), 0.0)
        total = zero
        for x in range(rows):
            n = padded[s, x + 1, 8 : cols + 8]
            beside = padded[s, x, 8 : cols + 8] + padded[s, x + 2, 8 : cols + 8]
            beside += padded[s, x + 1, 7 : cols + 7] + padded[s, x + 1, 9 : cols + 9]
            beside += jnp.where(lane == 0, 0.0, pltpu.roll(n, 1, 1))
            beside += jnp.where(lane == slab - 1, 0.0, pltpu.roll(n, slab - 1, 1))
            value = 6.0 * n - beside
            partial[s, x] = value
            total += value * value
        message[4 * owners + s : 4 * owners + s + 1] = jnp.sum(total, axis=0, keepdims=True)
        at = 4 * owners + shots + s
        message[at : at + 1] = jnp.full((1, slab), starts[s].astype(jnp.float32))
    for r in range(owners):
        for at, image, shift, top in ((0, padded, 1, 8), (2 * owners, partial, 0, 0)):
            held = [image[s, r * own + j + shift, top : top + cols] for s in range(shots) for j in range(own)]
            turned = jnp.concatenate(held, axis=0).T
            message[at + r : at + r + 1] = turned[0:1]
            message[at + owners + r : at + owners + r + 1] = turned[slab - 1 : slab]
    edges = message.shape[0]
    handed[0:edges] = message[...]
    mine, core = lax.axis_index("shot"), lax.axis_index("depth") % 2
    for k in range(owners // 2):
        r = partner_of(mine, 1 - core, k)
        for s in range(shots):
            for j in range(own):
                at = edges + (k * shots * own + s * own + j) * window
                handed[at : at + window] = partial[s, r * own + j, pl.ds(starts[s], window)]
    for k, block in early.items():
        r = partner_of(mine, core, k)
        for s in range(shots):
            for j in range(own):
                at = (s * own + j) * window
                block[at : at + window] = partial[s, r * own + j, pl.ds(starts[s], window)]


def finish_filter_kernel(ahead, partial, handed, messages, blocks, slabs_held, halo):
    shots, rows, cols, slab = partial.shape
    slabs = len(messages)
    edges, width = messages[0].shape
    own = width // (shots * cols)
    owners = rows // own
    half = owners // 2
    window = cols // 2 + 2
    sent = shots * own * window
    mine, here = lax.axis_index("shot"), lax.axis_index("depth")
    for k in range(slabs):
        slabs_held[here ^ k] = messages[k][...] if k != 1 else handed[0:edges]
    cross = jnp.zeros((owners, width), jnp.float32)
    for d in range(slabs - 1):
        right = slabs_held[d + 1, 0:owners]
        left = slabs_held[d, owners : 2 * owners]
        cross += right * (right - 2.0 * slabs_held[d, 3 * owners : 4 * owners])
        cross += left * (left - 2.0 * slabs_held[d + 1, 2 * owners : 3 * owners])
    cross = jnp.sum(cross, axis=0, keepdims=True)
    lane = lax.broadcasted_iota(jnp.int32, (1, width), 1)
    tails = []
    starts = []
    for s in range(shots):
        energy = jnp.where((lane >= s * own * cols) & (lane < (s + 1) * own * cols), cross, 0.0)
        for d in range(slabs):
            energy += slabs_held[d, 4 * owners + s : 4 * owners + s + 1]
        tails.append(energy)
        starts.append(jnp.max(messages[0][4 * owners + shots + s : 4 * owners + shots + s + 1]).astype(jnp.int32))
    tails.append(messages[0][4 * owners + shots :])
    tail = jnp.concatenate(tails, axis=0)
    depth = lax.broadcasted_iota(jnp.int32, (slab, width), 0)
    for whose in range(2):
        d = here ^ whose
        below = jnp.maximum(d - 1, 0)
        above = jnp.minimum(d + 1, slabs - 1)
        for k in range(half):
            r = partner_of(mine, here % 2, k)
            low = jnp.where(d > 0, slabs_held[below, pl.ds(owners + r, 1)], 0.0)
            high = jnp.where(d < slabs - 1, slabs_held[above, pl.ds(r, 1)], 0.0)
            if k in ahead and not whose:
                blocks[k][0:1] = low
                blocks[k][1:2] = high
                continue
            halo[whose, k] = jnp.where(depth == 0, low, jnp.where(depth == slab - 1, high, 0.0)).T
            for s in range(shots):
                for j in range(own):
                    i = s * own + j
                    if whose:
                        at = edges + (k * shots * own + i) * window
                        value = handed[at : at + window]
                        at = (2 if k in ahead else sent) + i * window
                    else:
                        value = partial[s, r * own + j, pl.ds(starts[s], window)]
                        at = i * window
                    blocks[k][at : at + window] = value - halo[whose, k, pl.ds(i * cols + starts[s], window)]
    for k in range(half):
        blocks[k][blocks[k].shape[0] - 2 * shots :] = tail


def combine_kernel(cells, total_shots, shots, parts, stack, weights, halo):
    own, cols, slab = stack.shape
    window = cols // 2 + 2
    tails = [block.shape[0] - 2 * shots for block, _, _ in parts]
    energy = jnp.concatenate([part[0][at : at + shots] for part, at in zip(parts, tails)], axis=0)
    meansq = jnp.sum(energy, axis=1, keepdims=True) / cells
    peak = jnp.max(meansq, axis=0, keepdims=True)
    weight = (1.0 / math.sqrt(total_shots)) / jnp.sqrt(meansq + 0.5 * peak + 1.0)
    weights[...] = jnp.broadcast_to(weight, weights.shape)
    stack[...] = jnp.zeros(stack.shape, jnp.float32)
    depth = lax.broadcasted_iota(jnp.int32, (slab, shots * own * cols), 0)
    for k, ((block, rows, early), tail) in enumerate(zip(parts, tails)):
        if early is not None:
            halo[k] = jnp.where(depth == 0, block[0:1], jnp.where(depth == slab - 1, block[1:2], 0.0)).T
        for s in range(shots):
            at = tail + shots + s
            start = jnp.max(block[at : at + 1]).astype(jnp.int32)
            scale = weights[k * shots + s : k * shots + s + 1]
            for j in range(own):
                i = s * own + j
                if early is not None:
                    value = early[i * window : (i + 1) * window] - halo[k, pl.ds(i * cols + start, window)]
                else:
                    value = block[rows + i * window : rows + (i + 1) * window]
                stack[j, pl.ds(start, window)] += scale * value


def in_hbm(array):
    return pltpu.with_memory_space_constraint(array, pltpu.HBM)


def in_vmem(array):
    return pltpu.with_memory_space_constraint(array, pltpu.VMEM)


def on_device(correlation, illumination, aperture):
    shots, rows, cols, slab = correlation.shape
    owners, slabs = lax.axis_size("shot"), lax.axis_size("depth")
    assert owners & (owners - 1) == 0 and slabs & (slabs - 1) == 0 and rows % owners == 0
    own = rows // owners
    width = shots * own * cols
    assert width == slab == 128
    half = owners // 2
    edges, window = 4 * owners + 2 * shots, cols // 2 + 2
    sent = shots * own * window
    f32 = jnp.float32
    vmem = pl.BlockSpec(memory_space=pltpu.VMEM)
    hbm = pl.BlockSpec(memory_space=pltpu.HBM)
    params = pltpu.CompilerParams(vmem_limit_bytes=24 << 20)
    ahead = early_rounds(owners)

    def local_body(aperture, correlation, illumination, partial, message, handed, *refs):
        early = dict(zip(ahead, refs))
        local_filter_kernel(aperture, correlation, illumination, partial, message, handed, early, *refs[len(ahead) :])

    partial, message, handed, *early = pl.pallas_call(
        local_body,
        out_shape=(
            pltpu.VMEM(correlation.shape, f32),
            pltpu.VMEM((edges, width), f32),
            pltpu.VMEM((edges + half * sent, width), f32),
            *(pltpu.VMEM((sent, width), f32) for _ in ahead),
        ),
        in_specs=[hbm, hbm, hbm],
        out_specs=(vmem,) * (3 + len(ahead)),
        scratch_shapes=[
            pltpu.VMEM((shots, rows + 2, cols + 16, slab), f32),
            pltpu.VMEM(correlation.shape, f32),
            pltpu.VMEM(correlation.shape, f32),
            pltpu.SMEM(aperture.shape, aperture.dtype),
            pltpu.SemaphoreType.DMA((2, shots)),
            pltpu.SemaphoreType.DMA,
        ],
        compiler_params=params,
        name="local_filter",
    )(in_hbm(aperture), in_hbm(correlation), in_hbm(illumination))

    def round_pairs(k):
        pairs = []
        for g in range(owners):
            for d in range(slabs):
                pairs.append((g * slabs + d, partner_of(g, d % 2, k) * slabs + d))
        return pairs

    messages = [message]
    for k in range(1, slabs):
        pairs = [(i, i ^ k) for i in range(slabs)]
        if k == 1:
            handed = lax.ppermute(handed, "depth", pairs)
            messages.append(message)
        else:
            messages.append(lax.ppermute(message, "depth", pairs))
    for at, k in enumerate(ahead):
        early[at] = lax.ppermute(early[at], ("shot", "depth"), round_pairs(k))

    def finish_body(partial, handed, *refs):
        finish_filter_kernel(
            ahead, partial, handed, (refs[0], None) + refs[1 : slabs - 1], refs[slabs - 1 : slabs - 1 + half], *refs[slabs - 1 + half :]
        )

    block = pltpu.VMEM((2 * sent + 2 * shots, slab), f32)
    light = pltpu.VMEM((2 + sent + 2 * shots, slab), f32)
    blocks = list(pl.pallas_call(
        finish_body,
        out_shape=tuple(light if k in ahead else block for k in range(half)),
        in_specs=[vmem] * (1 + slabs),
        out_specs=(vmem,) * half,
        scratch_shapes=[
            pltpu.VMEM((slabs,) + message.shape, f32),
            pltpu.VMEM((2, half, width, slab), f32),
        ],
        compiler_params=params,
        name="finish_filter",
    )(*(in_vmem(v) for v in (partial, handed, messages[0], *messages[2:]))))
    passed = []
    for k in range(half):
        blocks[k] = lax.ppermute(blocks[k], ("shot", "depth"), round_pairs(k))
        passed.append(lax.ppermute(blocks[k], "depth", [(i, i ^ 1) for i in range(slabs)]))
    cells = rows * cols * slab * slabs

    def combine_body(*refs):
        early = dict(zip(ahead, refs))
        ours, theirs, rest = (refs[len(ahead) + at :] for at in (0, half, owners))
        parts = [(ours[k], 0, early.get(k)) for k in range(half)]
        parts += [(theirs[k], 2 if k in early else sent, None) for k in range(half)]
        combine_kernel(cells, shots * owners, shots, parts, *rest)

    return pl.pallas_call(
        combine_body,
        out_shape=jax.ShapeDtypeStruct((own, cols, slab), f32),
        in_specs=[vmem] * (len(ahead) + owners),
        out_specs=vmem,
        scratch_shapes=[pltpu.VMEM((owners * shots, slab), f32), pltpu.VMEM((half, width, slab), f32)],
        compiler_params=params,
        name="combine",
    )(*(in_vmem(v) for v in early + blocks + passed))


def early_rounds(owners):
    return (owners // 2 - 2,)


def solution(mesh):
    return jax.shard_map(
        on_device,
        mesh=mesh,
        in_specs=(P("shot", None, None, "depth"), P("shot", None, None, "depth"), P("shot", None)),
        out_specs=P("shot", None, "depth"),
        check_vma=False,
    )
```

```python
import math

import jax
import jax.numpy as jnp
from jax import lax
from jax.experimental import pallas as pl
from jax.experimental.pallas import tpu as pltpu
from jax.sharding import PartitionSpec as P


def partner_of(here, core, k):
    return here ^ (2 * k + (core + k + k // 2) % 2)


def local_filter_kernel(
    aperture_hbm, correlation_hbm, illumination_hbm, partial, message, handed, early,
    padded, correlation, illumination, aperture, arrived, read,
):
    shots, rows, cols, slab = correlation.shape
    own = message.shape[1] // (shots * cols)
    owners = rows // own
    window = cols // 2 + 2
    boxes = pltpu.make_async_copy(aperture_hbm, aperture, read)
    boxes.start()
    copies = []
    for s in range(shots):
        copies.append((
            pltpu.make_async_copy(correlation_hbm.at[s], correlation.at[s], arrived.at[0, s]),
            pltpu.make_async_copy(illumination_hbm.at[s], illumination.at[s], arrived.at[1, s]),
        ))
        for copy in copies[s]:
            copy.start()
    second = lax.broadcasted_iota(jnp.int32, (cols, slab), 0)
    lane = lax.broadcasted_iota(jnp.int32, (cols, slab), 1)
    zero = jnp.zeros((cols, slab), jnp.float32)
    rim = jnp.zeros((cols + 16, slab), jnp.float32)
    boxes.wait()
    starts = [jnp.clip(aperture[s, 2] - 1, 0, cols - window) for s in range(shots)]
    for s in range(shots):
        padded[s, 0] = rim
        padded[s, rows + 1] = rim
        for x in range(rows):
            padded[s, x + 1, 0:8] = rim[0:8]
            padded[s, x + 1, cols + 8 : cols + 16] = rim[0:8]
        for copy in copies[s]:
            copy.wait()
        in_cols = (second >= aperture[s, 2]) & (second < aperture[s, 3])
        for x in range(rows):
            keep = in_cols & (x >= aperture[s, 0]) & (x < aperture[s, 1])
            padded[s, x + 1, 8 : cols + 8] = jnp.where(keep, correlation[s, x] / (illumination[s, x] + 0.1), 0.0)
        total = zero
        for x in range(rows):
            n = padded[s, x + 1, 8 : cols + 8]
            beside = padded[s, x, 8 : cols + 8] + padded[s, x + 2, 8 : cols + 8]
            beside += padded[s, x + 1, 7 : cols + 7] + padded[s, x + 1, 9 : cols + 9]
            beside += jnp.where(lane == 0, 0.0, pltpu.roll(n, 1, 1))
            beside += jnp.where(lane == slab - 1, 0.0, pltpu.roll(n, slab - 1, 1))
            value = 6.0 * n - beside
            partial[s, x] = value
            total += value * value
        message[4 * owners + s : 4 * owners + s + 1] = jnp.sum(total, axis=0, keepdims=True)
        at = 4 * owners + shots + s
        message[at : at + 1] = jnp.full((1, slab), starts[s].astype(jnp.float32))
    for r in range(owners):
        for at, image, shift, top in ((0, padded, 1, 8), (2 * owners, partial, 0, 0)):
            held = [image[s, r * own + j + shift, top : top + cols] for s in range(shots) for j in range(own)]
            turned = jnp.concatenate(held, axis=0).T
            message[at + r : at + r + 1] = turned[0:1]
            message[at + owners + r : at + owners + r + 1] = turned[slab - 1 : slab]
    edges = message.shape[0]
    handed[0:edges] = message[...]
    mine, core = lax.axis_index("shot"), lax.axis_index("depth") % 2
    for k in range(owners // 2):
        r = partner_of(mine, 1 - core, k)
        for s in range(shots):
            for j in range(own):
                at = edges + (k * shots * own + s * own + j) * window
                handed[at : at + window] = partial[s, r * own + j, pl.ds(starts[s], window)]
    for k, block in early.items():
        r = partner_of(mine, core, k)
        for s in range(shots):
            for j in range(own):
                at = (s * own + j) * window
                block[at : at + window] = partial[s, r * own + j, pl.ds(starts[s], window)]


def finish_filter_kernel(ahead, partial, handed, messages, blocks, slabs_held, halo):
    shots, rows, cols, slab = partial.shape
    slabs = len(messages)
    edges, width = messages[0].shape
    own = width // (shots * cols)
    owners = rows // own
    half = owners // 2
    window = cols // 2 + 2
    sent = shots * own * window
    mine, here = lax.axis_index("shot"), lax.axis_index("depth")
    for k in range(slabs):
        slabs_held[here ^ k] = messages[k][...] if k != 1 else handed[0:edges]
    cross = jnp.zeros((owners, width), jnp.float32)
    for d in range(slabs - 1):
        right = slabs_held[d + 1, 0:owners]
        left = slabs_held[d, owners : 2 * owners]
        cross += right * (right - 2.0 * slabs_held[d, 3 * owners : 4 * owners])
        cross += left * (left - 2.0 * slabs_held[d + 1, 2 * owners : 3 * owners])
    cross = jnp.sum(cross, axis=0, keepdims=True)
    lane = lax.broadcasted_iota(jnp.int32, (1, width), 1)
    tails = []
    starts = []
    for s in range(shots):
        energy = jnp.where((lane >= s * own * cols) & (lane < (s + 1) * own * cols), cross, 0.0)
        for d in range(slabs):
            energy += slabs_held[d, 4 * owners + s : 4 * owners + s + 1]
        tails.append(energy)
        starts.append(jnp.max(messages[0][4 * owners + shots + s : 4 * owners + shots + s + 1]).astype(jnp.int32))
    tails.append(messages[0][4 * owners + shots :])
    tail = jnp.concatenate(tails, axis=0)
    depth = lax.broadcasted_iota(jnp.int32, (slab, width), 0)
    for whose in range(2):
        d = here ^ whose
        below = jnp.maximum(d - 1, 0)
        above = jnp.minimum(d + 1, slabs - 1)
        for k in range(half):
            r = partner_of(mine, here % 2, k)
            low = jnp.where(d > 0, slabs_held[below, pl.ds(owners + r, 1)], 0.0)
            high = jnp.where(d < slabs - 1, slabs_held[above, pl.ds(r, 1)], 0.0)
            if k in ahead and not whose:
                blocks[k][0:1] = low
                blocks[k][1:2] = high
                continue
            halo[whose, k] = jnp.where(depth == 0, low, jnp.where(depth == slab - 1, high, 0.0)).T
            for s in range(shots):
                for j in range(own):
                    i = s * own + j
                    if whose:
                        at = edges + (k * shots * own + i) * window
                        value = handed[at : at + window]
                        at = (2 if k in ahead else sent) + i * window
                    else:
                        value = partial[s, r * own + j, pl.ds(starts[s], window)]
                        at = i * window
                    blocks[k][at : at + window] = value - halo[whose, k, pl.ds(i * cols + starts[s], window)]
    for k in range(half):
        blocks[k][blocks[k].shape[0] - 2 * shots :] = tail


def combine_kernel(cells, total_shots, shots, parts, stack, weights, halo, sums):
    own, cols, slab = stack.shape
    window = cols // 2 + 2
    tails = [block.shape[0] - 2 * shots for block, _, _ in parts]
    energy = jnp.concatenate([part[0][at : at + shots] for part, at in zip(parts, tails)], axis=0)
    meansq = jnp.sum(energy, axis=1, keepdims=True) / cells
    peak = jnp.max(meansq, axis=0, keepdims=True)
    weight = (1.0 / math.sqrt(total_shots)) / jnp.sqrt(meansq + 0.5 * peak + 1.0)
    weights[...] = jnp.broadcast_to(weight, weights.shape)
    sums[...] = jnp.zeros(sums.shape, jnp.float32)
    depth = lax.broadcasted_iota(jnp.int32, (slab, shots * own * cols), 0)
    for k, ((block, rows, early), tail) in enumerate(zip(parts, tails)):
        if early is not None:
            halo[k] = jnp.where(depth == 0, block[0:1], jnp.where(depth == slab - 1, block[1:2], 0.0)).T
        for s in range(shots):
            at = tail + shots + s
            start = jnp.max(block[at : at + 1]).astype(jnp.int32)
            scale = weights[k * shots + s : k * shots + s + 1]
            for j in range(own):
                i = s * own + j
                if early is not None:
                    value = early[i * window : (i + 1) * window] - halo[k, pl.ds(i * cols + start, window)]
                else:
                    value = block[rows + i * window : rows + (i + 1) * window]
                sums[k % 2, s, j, pl.ds(start, window)] += scale * value
    stack[...] = jnp.sum(sums[...], axis=(0, 1))


def in_hbm(array):
    return pltpu.with_memory_space_constraint(array, pltpu.HBM)


def in_vmem(array):
    return pltpu.with_memory_space_constraint(array, pltpu.VMEM)


def on_device(correlation, illumination, aperture):
    shots, rows, cols, slab = correlation.shape
    owners, slabs = lax.axis_size("shot"), lax.axis_size("depth")
    assert owners & (owners - 1) == 0 and slabs & (slabs - 1) == 0 and rows % owners == 0
    own = rows // owners
    width = shots * own * cols
    assert width == slab == 128
    half = owners // 2
    edges, window = 4 * owners + 2 * shots, cols // 2 + 2
    sent = shots * own * window
    f32 = jnp.float32
    vmem = pl.BlockSpec(memory_space=pltpu.VMEM)
    hbm = pl.BlockSpec(memory_space=pltpu.HBM)
    params = pltpu.CompilerParams(vmem_limit_bytes=24 << 20)
    ahead = early_rounds(owners)

    def local_body(aperture, correlation, illumination, partial, message, handed, *refs):
        early = dict(zip(ahead, refs))
        local_filter_kernel(aperture, correlation, illumination, partial, message, handed, early, *refs[len(ahead) :])

    partial, message, handed, *early = pl.pallas_call(
        local_body,
        out_shape=(
            pltpu.VMEM(correlation.shape, f32),
            pltpu.VMEM((edges, width), f32),
            pltpu.VMEM((edges + half * sent, width), f32),
            *(pltpu.VMEM((sent, width), f32) for _ in ahead),
        ),
        in_specs=[hbm, hbm, hbm],
        out_specs=(vmem,) * (3 + len(ahead)),
        scratch_shapes=[
            pltpu.VMEM((shots, rows + 2, cols + 16, slab), f32),
            pltpu.VMEM(correlation.shape, f32),
            pltpu.VMEM(correlation.shape, f32),
            pltpu.SMEM(aperture.shape, aperture.dtype),
            pltpu.SemaphoreType.DMA((2, shots)),
            pltpu.SemaphoreType.DMA,
        ],
        compiler_params=params,
        name="local_filter",
    )(in_hbm(aperture), in_hbm(correlation), in_hbm(illumination))

    def round_pairs(k):
        pairs = []
        for g in range(owners):
            for d in range(slabs):
                pairs.append((g * slabs + d, partner_of(g, d % 2, k) * slabs + d))
        return pairs

    messages = [message]
    for k in range(1, slabs):
        pairs = [(i, i ^ k) for i in range(slabs)]
        if k == 1:
            handed = lax.ppermute(handed, "depth", pairs)
            messages.append(message)
        else:
            messages.append(lax.ppermute(message, "depth", pairs))
    for at, k in enumerate(ahead):
        early[at] = lax.ppermute(early[at], ("shot", "depth"), round_pairs(k))

    def finish_body(partial, handed, *refs):
        finish_filter_kernel(
            ahead, partial, handed, (refs[0], None) + refs[1 : slabs - 1], refs[slabs - 1 : slabs - 1 + half], *refs[slabs - 1 + half :]
        )

    block = pltpu.VMEM((2 * sent + 2 * shots, slab), f32)
    light = pltpu.VMEM((2 + sent + 2 * shots, slab), f32)
    blocks = list(pl.pallas_call(
        finish_body,
        out_shape=tuple(light if k in ahead else block for k in range(half)),
        in_specs=[vmem] * (1 + slabs),
        out_specs=(vmem,) * half,
        scratch_shapes=[
            pltpu.VMEM((slabs,) + message.shape, f32),
            pltpu.VMEM((2, half, width, slab), f32),
        ],
        compiler_params=params,
        name="finish_filter",
    )(*(in_vmem(v) for v in (partial, handed, messages[0], *messages[2:]))))
    passed = []
    for k in range(half):
        blocks[k] = lax.ppermute(blocks[k], ("shot", "depth"), round_pairs(k))
        passed.append(lax.ppermute(blocks[k], "depth", [(i, i ^ 1) for i in range(slabs)]))
    cells = rows * cols * slab * slabs

    def combine_body(*refs):
        early = dict(zip(ahead, refs))
        ours, theirs, rest = (refs[len(ahead) + at :] for at in (0, half, owners))
        parts = [(ours[k], 0, early.get(k)) for k in range(half)]
        parts += [(theirs[k], 2 if k in early else sent, None) for k in range(half)]
        combine_kernel(cells, shots * owners, shots, parts, *rest)

    return pl.pallas_call(
        combine_body,
        out_shape=jax.ShapeDtypeStruct((own, cols, slab), f32),
        in_specs=[vmem] * (len(ahead) + owners),
        out_specs=vmem,
        scratch_shapes=[pltpu.VMEM((owners * shots, slab), f32), pltpu.VMEM((half, width, slab), f32),
            pltpu.VMEM((2, shots, own, cols, slab), f32),
        ],
        compiler_params=params,
        name="combine",
    )(*(in_vmem(v) for v in early + blocks + passed))


def early_rounds(owners):
    return (owners // 2 - 2,)


def solution(mesh):
    return jax.shard_map(
        on_device,
        mesh=mesh,
        in_specs=(P("shot", None, None, "depth"), P("shot", None, None, "depth"), P("shot", None)),
        out_specs=P("shot", None, "depth"),
        check_vma=False,
    )
```

```python
import math

import jax
import jax.numpy as jnp
from jax import lax
from jax.experimental import pallas as pl
from jax.experimental.pallas import tpu as pltpu
from jax.sharding import PartitionSpec as P


def partner_of(here, core, k):
    return here ^ (2 * k + (core + k + k // 2) % 2)


def local_filter_kernel(
    aperture_hbm, correlation_hbm, illumination_hbm, partial, message,
    padded, correlation, illumination, aperture, arrived, read,
):
    shots, rows, cols, slab = correlation.shape
    own = message.shape[1] // (shots * cols)
    owners = rows // own
    window = cols // 2 + 2
    boxes = pltpu.make_async_copy(aperture_hbm, aperture, read)
    boxes.start()
    copies = []
    for s in range(shots):
        copies.append((
            pltpu.make_async_copy(correlation_hbm.at[s], correlation.at[s], arrived.at[0, s]),
            pltpu.make_async_copy(illumination_hbm.at[s], illumination.at[s], arrived.at[1, s]),
        ))
        for copy in copies[s]:
            copy.start()
    second = lax.broadcasted_iota(jnp.int32, (cols, slab), 0)
    lane = lax.broadcasted_iota(jnp.int32, (cols, slab), 1)
    zero = jnp.zeros((cols, slab), jnp.float32)
    rim = jnp.zeros((cols + 16, slab), jnp.float32)
    boxes.wait()
    starts = [jnp.clip(aperture[s, 2] - 1, 0, cols - window) for s in range(shots)]
    for s in range(shots):
        padded[s, 0] = rim
        padded[s, rows + 1] = rim
        for x in range(rows):
            padded[s, x + 1, 0:8] = rim[0:8]
            padded[s, x + 1, cols + 8 : cols + 16] = rim[0:8]
        for copy in copies[s]:
            copy.wait()
        in_cols = (second >= aperture[s, 2]) & (second < aperture[s, 3])
        for x in range(rows):
            keep = in_cols & (x >= aperture[s, 0]) & (x < aperture[s, 1])
            padded[s, x + 1, 8 : cols + 8] = jnp.where(keep, correlation[s, x] / (illumination[s, x] + 0.1), 0.0)
        total = zero
        for x in range(rows):
            n = padded[s, x + 1, 8 : cols + 8]
            beside = padded[s, x, 8 : cols + 8] + padded[s, x + 2, 8 : cols + 8]
            beside += padded[s, x + 1, 7 : cols + 7] + padded[s, x + 1, 9 : cols + 9]
            beside += jnp.where(lane == 0, 0.0, pltpu.roll(n, 1, 1))
            beside += jnp.where(lane == slab - 1, 0.0, pltpu.roll(n, slab - 1, 1))
            value = 6.0 * n - beside
            partial[s, x] = value
            total += value * value
        message[4 * owners + s : 4 * owners + s + 1] = jnp.sum(total, axis=0, keepdims=True)
        at = 4 * owners + shots + s
        message[at : at + 1] = jnp.full((1, slab), starts[s].astype(jnp.float32))
    for r in range(owners):
        for at, image, shift, top in ((0, padded, 1, 8), (2 * owners, partial, 0, 0)):
            held = [image[s, r * own + j + shift, top : top + cols] for s in range(shots) for j in range(own)]
            turned = jnp.concatenate(held, axis=0).T
            message[at + r : at + r + 1] = turned[0:1]
            message[at + owners + r : at + owners + r + 1] = turned[slab - 1 : slab]


def windows_kernel(partial, message, handed, early):
    shots, rows, cols, _ = partial.shape
    own = message.shape[1] // (shots * cols)
    owners = rows // own
    window = cols // 2 + 2
    at = 4 * owners + shots
    starts = [jnp.max(message[at + s : at + s + 1]).astype(jnp.int32) for s in range(shots)]
    edges = message.shape[0]
    handed[0:edges] = message[...]
    mine, core = lax.axis_index("shot"), lax.axis_index("depth") % 2
    for k in range(owners // 2):
        r = partner_of(mine, 1 - core, k)
        for s in range(shots):
            for j in range(own):
                at = edges + (k * shots * own + s * own + j) * window
                handed[at : at + window] = partial[s, r * own + j, pl.ds(starts[s], window)]
    for k, block in early.items():
        r = partner_of(mine, core, k)
        for s in range(shots):
            for j in range(own):
                at = (s * own + j) * window
                block[at : at + window] = partial[s, r * own + j, pl.ds(starts[s], window)]


def finish_filter_kernel(ahead, partial, handed, messages, blocks, slabs_held, halo):
    shots, rows, cols, slab = partial.shape
    slabs = len(messages)
    edges, width = messages[0].shape
    own = width // (shots * cols)
    owners = rows // own
    half = owners // 2
    window = cols // 2 + 2
    sent = shots * own * window
    mine, here = lax.axis_index("shot"), lax.axis_index("depth")
    for k in range(slabs):
        slabs_held[here ^ k] = messages[k][...] if k != 1 else handed[0:edges]
    cross = jnp.zeros((owners, width), jnp.float32)
    for d in range(slabs - 1):
        right = slabs_held[d + 1, 0:owners]
        left = slabs_held[d, owners : 2 * owners]
        cross += right * (right - 2.0 * slabs_held[d, 3 * owners : 4 * owners])
        cross += left * (left - 2.0 * slabs_held[d + 1, 2 * owners : 3 * owners])
    cross = jnp.sum(cross, axis=0, keepdims=True)
    lane = lax.broadcasted_iota(jnp.int32, (1, width), 1)
    tails = []
    starts = []
    for s in range(shots):
        energy = jnp.where((lane >= s * own * cols) & (lane < (s + 1) * own * cols), cross, 0.0)
        for d in range(slabs):
            energy += slabs_held[d, 4 * owners + s : 4 * owners + s + 1]
        tails.append(energy)
        starts.append(jnp.max(messages[0][4 * owners + shots + s : 4 * owners + shots + s + 1]).astype(jnp.int32))
    tails.append(messages[0][4 * owners + shots :])
    tail = jnp.concatenate(tails, axis=0)
    depth = lax.broadcasted_iota(jnp.int32, (slab, width), 0)
    for whose in range(2):
        d = here ^ whose
        below = jnp.maximum(d - 1, 0)
        above = jnp.minimum(d + 1, slabs - 1)
        for k in range(half):
            r = partner_of(mine, here % 2, k)
            low = jnp.where(d > 0, slabs_held[below, pl.ds(owners + r, 1)], 0.0)
            high = jnp.where(d < slabs - 1, slabs_held[above, pl.ds(r, 1)], 0.0)
            if k in ahead and not whose:
                blocks[k][0:1] = low
                blocks[k][1:2] = high
                continue
            halo[whose, k] = jnp.where(depth == 0, low, jnp.where(depth == slab - 1, high, 0.0)).T
            for s in range(shots):
                for j in range(own):
                    i = s * own + j
                    if whose:
                        at = edges + (k * shots * own + i) * window
                        value = handed[at : at + window]
                        at = (2 if k in ahead else sent) + i * window
                    else:
                        value = partial[s, r * own + j, pl.ds(starts[s], window)]
                        at = i * window
                    blocks[k][at : at + window] = value - halo[whose, k, pl.ds(i * cols + starts[s], window)]
    for k in range(half):
        blocks[k][blocks[k].shape[0] - 2 * shots :] = tail


def combine_kernel(cells, total_shots, shots, parts, stack, weights, halo, sums):
    own, cols, slab = stack.shape
    window = cols // 2 + 2
    tails = [block.shape[0] - 2 * shots for block, _, _ in parts]
    energy = jnp.concatenate([part[0][at : at + shots] for part, at in zip(parts, tails)], axis=0)
    meansq = jnp.sum(energy, axis=1, keepdims=True) / cells
    peak = jnp.max(meansq, axis=0, keepdims=True)
    weight = (1.0 / math.sqrt(total_shots)) / jnp.sqrt(meansq + 0.5 * peak + 1.0)
    weights[...] = jnp.broadcast_to(weight, weights.shape)
    sums[...] = jnp.zeros(sums.shape, jnp.float32)
    depth = lax.broadcasted_iota(jnp.int32, (slab, shots * own * cols), 0)
    for k, ((block, rows, early), tail) in enumerate(zip(parts, tails)):
        if early is not None:
            halo[k] = jnp.where(depth == 0, block[0:1], jnp.where(depth == slab - 1, block[1:2], 0.0)).T
        for s in range(shots):
            at = tail + shots + s
            start = jnp.max(block[at : at + 1]).astype(jnp.int32)
            scale = weights[k * shots + s : k * shots + s + 1]
            for j in range(own):
                i = s * own + j
                if early is not None:
                    value = early[i * window : (i + 1) * window] - halo[k, pl.ds(i * cols + start, window)]
                else:
                    value = block[rows + i * window : rows + (i + 1) * window]
                sums[k % 2, s, j, pl.ds(start, window)] += scale * value
    stack[...] = jnp.sum(sums[...], axis=(0, 1))


def in_hbm(array):
    return pltpu.with_memory_space_constraint(array, pltpu.HBM)


def in_vmem(array):
    return pltpu.with_memory_space_constraint(array, pltpu.VMEM)


def on_device(correlation, illumination, aperture):
    shots, rows, cols, slab = correlation.shape
    owners, slabs = lax.axis_size("shot"), lax.axis_size("depth")
    assert owners & (owners - 1) == 0 and slabs & (slabs - 1) == 0 and rows % owners == 0
    own = rows // owners
    width = shots * own * cols
    assert width == slab == 128
    half = owners // 2
    edges, window = 4 * owners + 2 * shots, cols // 2 + 2
    sent = shots * own * window
    f32 = jnp.float32
    vmem = pl.BlockSpec(memory_space=pltpu.VMEM)
    hbm = pl.BlockSpec(memory_space=pltpu.HBM)
    params = pltpu.CompilerParams(vmem_limit_bytes=24 << 20)
    ahead = early_rounds(owners)

    partial, message = pl.pallas_call(
        local_filter_kernel,
        out_shape=(
            pltpu.VMEM(correlation.shape, f32),
            pltpu.VMEM((edges, width), f32),
        ),
        in_specs=[hbm, hbm, hbm],
        out_specs=(vmem, vmem),
        scratch_shapes=[
            pltpu.VMEM((shots, rows + 2, cols + 16, slab), f32),
            pltpu.VMEM(correlation.shape, f32),
            pltpu.VMEM(correlation.shape, f32),
            pltpu.SMEM(aperture.shape, aperture.dtype),
            pltpu.SemaphoreType.DMA((2, shots)),
            pltpu.SemaphoreType.DMA,
        ],
        compiler_params=params,
        name="local_filter",
    )(in_hbm(aperture), in_hbm(correlation), in_hbm(illumination))

    def windows_body(partial, message, handed, *refs):
        windows_kernel(partial, message, handed, dict(zip(ahead, refs)))

    handed, *early = pl.pallas_call(
        windows_body,
        out_shape=(
            pltpu.VMEM((edges + half * sent, width), f32),
            *(pltpu.VMEM((sent, width), f32) for _ in ahead),
        ),
        in_specs=[vmem, vmem],
        out_specs=(vmem,) * (1 + len(ahead)),
        compiler_params=params,
        name="windows",
    )(in_vmem(partial), in_vmem(message))

    def round_pairs(k):
        pairs = []
        for g in range(owners):
            for d in range(slabs):
                pairs.append((g * slabs + d, partner_of(g, d % 2, k) * slabs + d))
        return pairs

    messages = [message]
    for k in range(1, slabs):
        pairs = [(i, i ^ k) for i in range(slabs)]
        if k == 1:
            handed = lax.ppermute(handed, "depth", pairs)
            messages.append(message)
        else:
            messages.append(lax.ppermute(message, "depth", pairs))
    for at, k in enumerate(ahead):
        early[at] = lax.ppermute(early[at], ("shot", "depth"), round_pairs(k))

    def finish_body(partial, handed, *refs):
        finish_filter_kernel(
            ahead, partial, handed, (refs[0], None) + refs[1 : slabs - 1], refs[slabs - 1 : slabs - 1 + half], *refs[slabs - 1 + half :]
        )

    block = pltpu.VMEM((2 * sent + 2 * shots, slab), f32)
    light = pltpu.VMEM((2 + sent + 2 * shots, slab), f32)
    blocks = list(pl.pallas_call(
        finish_body,
        out_shape=tuple(light if k in ahead else block for k in range(half)),
        in_specs=[vmem] * (1 + slabs),
        out_specs=(vmem,) * half,
        scratch_shapes=[
            pltpu.VMEM((slabs,) + message.shape, f32),
            pltpu.VMEM((2, half, width, slab), f32),
        ],
        compiler_params=params,
        name="finish_filter",
    )(*(in_vmem(v) for v in (partial, handed, messages[0], *messages[2:]))))
    passed = []
    for k in range(half):
        blocks[k] = lax.ppermute(blocks[k], ("shot", "depth"), round_pairs(k))
        passed.append(lax.ppermute(blocks[k], "depth", [(i, i ^ 1) for i in range(slabs)]))
    cells = rows * cols * slab * slabs

    def combine_body(*refs):
        early = dict(zip(ahead, refs))
        ours, theirs, rest = (refs[len(ahead) + at :] for at in (0, half, owners))
        parts = [(ours[k], 0, early.get(k)) for k in range(half)]
        parts += [(theirs[k], 2 if k in early else sent, None) for k in range(half)]
        combine_kernel(cells, shots * owners, shots, parts, *rest)

    return pl.pallas_call(
        combine_body,
        out_shape=jax.ShapeDtypeStruct((own, cols, slab), f32),
        in_specs=[vmem] * (len(ahead) + owners),
        out_specs=vmem,
        scratch_shapes=[pltpu.VMEM((owners * shots, slab), f32), pltpu.VMEM((half, width, slab), f32),
            pltpu.VMEM((2, shots, own, cols, slab), f32),
        ],
        compiler_params=params,
        name="combine",
    )(*(in_vmem(v) for v in early + blocks + passed))


def early_rounds(owners):
    return (owners // 2 - 2,)


def solution(mesh):
    return jax.shard_map(
        on_device,
        mesh=mesh,
        in_specs=(P("shot", None, None, "depth"), P("shot", None, None, "depth"), P("shot", None)),
        out_specs=P("shot", None, "depth"),
        check_vma=False,
    )
```
